32 devices in a mesh: dp: 8 (over z, x), seq: 4 (over y, core).
Axes of the slice: x: 2, y: 2, z: 4, core: 2. Of those that a mesh axis runs over, the one named last changes fastest.
Arguments:
- queries: bfloat16 [8, 512, 2048], P('dp', 'seq'), may hold values from -5 to 5
- key_states: bfloat16 [8, 512, 2048], P('dp', 'seq'), may hold values from -5 to 5
- value_states: bfloat16 [8, 512, 2048], P('dp', 'seq'), may hold values from -6 to 6
- residual: bfloat16 [8, 512, 2048], P('dp', 'seq'), may hold values from -6 to 6
- enc_hidden: bfloat16 [8, 512, 1536], P('dp', 'seq'), may hold values from -6 to 6
- enc_gain: float32 [1536], replicated, may hold values from 0.1 to 1.9
- enc_bias: float32 [1536], replicated, may hold values from -0.5 to 0.5
- feature_target: int32 [8, 512], P('dp', 'seq'), may hold values from 0 to 511, as said below
- timestep: int32 [8], P('dp'), may hold values from 0 to 999
- gate_weight: bfloat16 [256, 2048], P('dp'), may hold values from -0.375 to 0.375
- lift_weight: bfloat16 [2048, 1024], P('dp'), may hold values from -0.125 to 0.125
- out_weight: bfloat16 [1024, 1536], P('dp'), may hold values from -0.1875 to 0.1875
Outputs:
- d_queries: bfloat16 [8, 512, 2048], P('dp', 'seq')
- d_keys: bfloat16 [8, 512, 2048], P('dp', 'seq')
- d_values: bfloat16 [8, 512, 2048], P('dp', 'seq')
- grad_gate: float32 [256, 2048], P('dp')
- grad_lift: float32 [2048, 1024], P('dp')
- grad_out: float32 [1024, 1536], P('dp')
The draws below stay inside these ranges and needn't reach their ends.
Inputs may be any that keep to these rules, and one draw needn't show every extreme that they name: For each clip, feature_target is a permutation of its 512 token positions. The 128 encoder rows of one device of seq target at most 64 tokens held by any one device of seq, and exactly 64 for some.
All inputs are finite; a program needn't handle non-finite values.
Results may differ from the reference program's by a relative error of at most 0.02.
Values may be sent and summed in bfloat16 or wider, within the bound.
No kernel may reach another device: no remote copies, remote signals or barrier semaphores. Data moves between devices by JAX's collectives and lax.ppermute only.
A program may use at most 128 MiB of HBM per device.

```python
import math
import jax
import jax.numpy as jnp
from jax import lax

TOK_DEV = 128
HEADS = 16
HD = 128
PH = 1024
ZD = 1536
TEMB = 256
CLIPS = 8
LEN = 512
FEAT = 2048


def pattern_draw(key, which):
    own = jax.random.fold_in(key, which)
    values = jnp.clip(jax.random.normal(own, (CLIPS, LEN, FEAT), jnp.float32), -5.0, 5.0)
    return values.astype(jnp.bfloat16)


def draw_queries(key, part):
    return pattern_draw(key, 1)


def draw_key_states(key, part):
    return pattern_draw(key, 2)


def draw_feature_target(key, part):
    groups = LEN // TOK_DEV
    share = TOK_DEV // groups

    def one_clip(clip_key):
        first = jax.random.fold_in(clip_key, 1)
        second = jax.random.fold_in(clip_key, 2)
        third = jax.random.fold_in(clip_key, 3)
        fourth = jax.random.fold_in(clip_key, 4)
        primary = jax.random.permutation(first, groups)
        offset = jax.random.randint(second, (), 1, groups)
        lesser = (primary + offset) % groups
        devices = jnp.arange(groups)
        counts = share + share * (devices[None, :] == primary[:, None]).astype(jnp.int32) - share * (devices[None, :] == lesser[:, None]).astype(jnp.int32)
        bounds = jnp.cumsum(counts, axis=1)
        slots = jnp.arange(TOK_DEV)
        owning = jnp.sum((bounds[:, None, :] <= slots[None, :, None]).astype(jnp.int32), axis=2)
        shuffle = jax.vmap(lambda sub_key: jax.random.permutation(sub_key, TOK_DEV))(jax.random.split(third, groups))
        owning = jnp.take_along_axis(owning, shuffle, axis=1).reshape(LEN)
        positions = jnp.arange(LEN)
        ranked = jnp.argsort(owning * LEN + positions, stable=True)
        within = jax.vmap(lambda sub_key: jax.random.permutation(sub_key, TOK_DEV))(jax.random.split(fourth, groups)).reshape(LEN)
        placed = positions // TOK_DEV * TOK_DEV + within
        return jnp.zeros((LEN,), jnp.int32).at[ranked].set(placed.astype(jnp.int32))
    return jax.vmap(one_clip)(jax.random.split(key, CLIPS))


def set_ends(entries, key, low, largest):
    dims = entries.shape
    spot = [jax.random.randint(jax.random.fold_in(key, axis), (), 0, dims[axis]) for axis in range(len(dims))]
    entries = entries.at[tuple(spot)].set(low)
    longest = dims.index(max(dims))
    spot[longest] = (spot[longest] + 1) % dims[longest]
    return entries.at[tuple(spot)].set(largest)


def strengthened(result, key, source, target, blocks, factor):
    def block_of(dim):
        return (jnp.arange(result.shape[dim]) // (result.shape[dim] // blocks)).reshape((-1,) + (1,) * (result.ndim - 1 - dim))

    one_side = jax.random.permutation(key, blocks)[block_of(target)]
    second = (block_of(target) + blocks // 2) % blocks
    return jnp.where((block_of(source) == one_side) | (block_of(source) == second), factor * result, result)


def level_of(rng, dims, cuts, least, largest):
    level, own = 1.0, jax.random.fold_in(rng, 6)
    for dim, blocks in cuts:
        heights = jnp.exp(jax.random.uniform(jax.random.fold_in(own, dim), (blocks,), jnp.float32, least / len(cuts), largest / len(cuts)))
        level = level * jnp.repeat(heights, dims[dim] // blocks).reshape([-1 if axis == dim else 1 for axis in range(len(dims))])
    return level


def noise(own_key, dims, deviation, limit, cuts=(), kind=jnp.bfloat16):
    values = deviation * jax.random.normal(own_key, dims, jnp.float32)
    if cuts:
        values = values * level_of(own_key, dims, cuts, -0.22, 0.18)
    return jnp.clip(values, -limit, limit).astype(kind)


def noise_with(rng, extent, scale, most, cuts, heavy, dtype=jnp.bfloat16):
    drawn = scale * jax.random.normal(rng, extent, jnp.float32)
    if cuts:
        drawn = drawn * level_of(rng, extent, cuts, -0.22, 0.18)
    return jnp.clip(strengthened(drawn, jax.random.fold_in(rng, 3), *heavy), -most, most).astype(dtype)


def setup_inputs(seed: int = 0) -> dict:
    key_of = jax.random.split(jax.random.key(seed), 13)
    queries = draw_queries(jax.random.fold_in(key_of[12], 71), 0)
    key_states = draw_key_states(jax.random.fold_in(key_of[12], 71), 0)
    value_states = noise(key_of[2], (CLIPS, LEN, FEAT), 1.0, 6.0, ((0, 8), (1, 4)))
    residual = noise_with(key_of[3], (CLIPS, LEN, FEAT), 1.0, 6.0, ((0, 8), (1, 4)), (0, 2, 8, 2.0))
    enc_hidden = noise(key_of[4], (CLIPS, LEN, ZD), 1.0, 6.0, ((0, 8), (1, 4)))
    enc_gain = jnp.clip(1.0 + 0.18 * jax.random.normal(key_of[5], (ZD,), jnp.float32), 0.1, 1.9)
    enc_bias = jnp.clip(jax.random.uniform(key_of[6], (ZD,), jnp.float32, -0.5, 0.5), -0.5, 0.5)
    feature_target = draw_feature_target(jax.random.fold_in(key_of[12], 71), 0)
    timestep = set_ends(jax.random.randint(key_of[8], (CLIPS,), 0, 1000), jax.random.fold_in(key_of[8], 1), 0, 999).astype(jnp.int32)
    gate_weight = noise(key_of[9], (TEMB, FEAT), TEMB ** -0.5, 0.375, ((0, 8),))
    lift_weight = noise(key_of[10], (FEAT, PH), FEAT ** -0.5, 0.125, ((0, 8),))
    out_weight = noise(key_of[11], (PH, ZD), PH ** -0.5, 0.1875, ((0, 8),))
    return {"queries": queries, "key_states": key_states, "value_states": value_states, "residual": residual, "enc_hidden": enc_hidden, "enc_gain": enc_gain, "enc_bias": enc_bias, "feature_target": feature_target, "timestep": timestep, "gate_weight": gate_weight, "lift_weight": lift_weight, "out_weight": out_weight}


EPSILON = 1e-06

def rounded(array):
    return lax.optimization_barrier(array.astype(jnp.bfloat16)).astype(jnp.float32)

def embed_time(timestep):
    half_width = TEMB // 2
    frequency = jnp.exp(-math.log(10000.0) * jnp.arange(half_width).astype(jnp.float32) / half_width)
    angles = timestep.astype(jnp.float32)[:, None] * frequency[None, :]
    return jnp.concatenate([jnp.cos(angles), jnp.sin(angles)], axis=1).astype(jnp.bfloat16)

def encoder_norm(hidden, enc_gain, enc_bias):
    widened = hidden.astype(jnp.float32)
    centred = widened - lax.optimization_barrier(jnp.mean(widened, axis=-1, keepdims=True))
    variance = lax.optimization_barrier(jnp.mean(centred * centred, axis=-1, keepdims=True))
    return (centred * lax.rsqrt(variance + EPSILON) * enc_gain + enc_bias).astype(jnp.bfloat16)

def soft_scores(query_block, key_heads):
    scores = jnp.einsum('bhd,lhd->hbl', query_block.astype(jnp.float32), key_heads.astype(jnp.float32)) * HD ** (-0.5)
    shifted = jnp.exp(scores - lax.optimization_barrier(jnp.max(scores, axis=-1, keepdims=True)))
    return shifted / lax.optimization_barrier(jnp.sum(shifted, axis=-1, keepdims=True))

def split_blocks(array):
    length = array.shape[0]
    block_rows = min(length, 512)
    return array.reshape(length // block_rows, block_rows, array.shape[1], array.shape[2])

def attention_forward(query_heads, key_heads, value_heads):

    def one_block(query_block):
        chances = rounded(soft_scores(query_block, key_heads))
        return jnp.einsum('hbl,lhd->bhd', chances, value_heads.astype(jnp.float32)).astype(jnp.bfloat16)
    mixed = lax.map(one_block, split_blocks(query_heads))
    return mixed.reshape(query_heads.shape[0], -1)

def attention_backward(query_heads, key_heads, value_heads, grad_heads):
    key_wide = key_heads.astype(jnp.float32)
    value_wide = value_heads.astype(jnp.float32)

    def one_block(carried, pieces):
        grad_keys, grad_values = carried
        query_block, grad_block = pieces
        chances = soft_scores(query_block, key_heads)
        grad_wide = grad_block.astype(jnp.float32)
        grad_chances = jnp.einsum('bhd,lhd->hbl', grad_wide, value_wide)
        grad_values = grad_values + jnp.einsum('hbl,bhd->lhd', rounded(chances), grad_wide)
        inner_sum = lax.optimization_barrier(jnp.sum(grad_chances * chances, axis=-1, keepdims=True))
        grad_scores = rounded(chances * (grad_chances - inner_sum) * HD ** (-0.5))
        grad_query = jnp.einsum('hbl,lhd->bhd', grad_scores, key_wide)
        grad_keys = grad_keys + jnp.einsum('hbl,bhd->lhd', grad_scores, query_block.astype(jnp.float32))
        return ((grad_keys, grad_values), grad_query.astype(jnp.bfloat16))
    zeros = jnp.zeros(key_heads.shape, jnp.float32)
    carried, grad_queries = lax.scan(one_block, (zeros, zeros), (split_blocks(query_heads), split_blocks(grad_heads)))
    length = query_heads.shape[0]
    return (grad_queries.reshape(length, -1), carried[0].reshape(length, -1).astype(jnp.bfloat16), carried[1].reshape(length, -1).astype(jnp.bfloat16))

def heads_of(array):
    return array.reshape(array.shape[0], HEADS, HD)

def reference(queries, key_states, value_states, residual, enc_hidden, enc_gain, enc_bias, feature_target, timestep, gate_weight, lift_weight, out_weight):
    embedded = embed_time(timestep)
    gating = jnp.dot(embedded, gate_weight, preferred_element_type=jnp.float32)
    normed = encoder_norm(enc_hidden, enc_gain, enc_bias)

    def place(feature_rows, target_rows):
        return jnp.zeros_like(feature_rows).at[target_rows].set(feature_rows)
    aligned = jax.vmap(place)(normed, feature_target)

    def clip_forward(triple):
        return attention_forward(heads_of(triple[0]), heads_of(triple[1]), heads_of(triple[2]))
    mixed = lax.map(clip_forward, (queries, key_states, value_states))
    hidden = (residual.astype(jnp.float32) + gating[:, None, :] * mixed.astype(jnp.float32)).astype(jnp.bfloat16)
    flat_hidden = hidden.reshape(-1, HEADS * HD)
    lifted = jnp.dot(flat_hidden, lift_weight, preferred_element_type=jnp.float32)
    sigmoid_lift = jax.nn.sigmoid(lifted)
    activated = (lifted * sigmoid_lift).astype(jnp.bfloat16)
    predicted = jnp.dot(activated, out_weight, preferred_element_type=jnp.float32)
    target_wide = aligned.reshape(-1, ZD).astype(jnp.float32)
    pred_norm = jnp.sqrt(lax.optimization_barrier(jnp.sum(predicted * predicted, axis=1, keepdims=True)) + EPSILON)
    target_norm = jnp.sqrt(lax.optimization_barrier(jnp.sum(target_wide * target_wide, axis=1, keepdims=True)) + EPSILON)
    cosine = lax.optimization_barrier(jnp.sum(predicted * target_wide, axis=1, keepdims=True)) / (pred_norm * target_norm)
    grad_pred = (-1.0 * ZD * (target_wide / (pred_norm * target_norm) - cosine * predicted / (pred_norm * pred_norm))).astype(jnp.bfloat16)
    grad_out = jnp.dot(activated.T, grad_pred, preferred_element_type=jnp.float32)
    grad_act = jnp.dot(grad_pred, out_weight.T, preferred_element_type=jnp.float32)
    grad_lifted = (grad_act * sigmoid_lift * (1.0 + lifted * (1.0 - sigmoid_lift))).astype(jnp.bfloat16)
    grad_lift = jnp.dot(flat_hidden.T, grad_lifted, preferred_element_type=jnp.float32)
    grad_hidden = jnp.dot(grad_lifted, lift_weight.T, preferred_element_type=jnp.float32).reshape(CLIPS, LEN, HEADS * HD)
    grad_mixed = (gating[:, None, :] * grad_hidden).astype(jnp.bfloat16)
    grad_gating = lax.optimization_barrier(jnp.sum(grad_hidden * mixed.astype(jnp.float32), axis=1))
    grad_gate = jnp.dot(embedded.astype(jnp.float32).T, grad_gating, precision=lax.Precision.HIGHEST)

    def clip_backward(quad):
        return attention_backward(heads_of(quad[0]), heads_of(quad[1]), heads_of(quad[2]), heads_of(quad[3]))
    back = lax.map(clip_backward, (queries, key_states, value_states, grad_mixed))
    return (back[0], back[1], back[2], grad_gate, grad_lift, grad_out)
```

```python
import functools
import math

import jax
import jax.numpy as jnp
from jax import lax
from jax.experimental import pallas as pl
from jax.experimental.pallas import tpu as pltpu
from jax.sharding import PartitionSpec as P

HD = 128
EPSILON = 1e-06
BF = jnp.bfloat16
F32 = jnp.float32


def embed_time(timestep, width):
    half_width = width // 2
    frequency = jnp.exp(
        -math.log(10000.0) * jnp.arange(half_width).astype(F32) / half_width
    )
    angles = timestep.astype(F32)[:, None] * frequency[None, :]
    return jnp.concatenate([jnp.cos(angles), jnp.sin(angles)], axis=1).astype(BF)


def nt(a, b):
    return lax.dot_general(a, b, (((1,), (1,)), ((), ())), preferred_element_type=F32)


def nn(a, b):
    return lax.dot_general(a, b, (((1,), (0,)), ((), ())), preferred_element_type=F32)


def tn(a, b):
    return lax.dot_general(a, b, (((0,), (0,)), ((), ())), preferred_element_type=F32)


def forward_body(blocks, *refs):
    packs, outs = refs[:blocks], refs[blocks:]
    keys = jnp.concatenate([p[1] for p in packs], axis=0)
    values = jnp.concatenate([p[2] for p in packs], axis=0)
    for pack, out in zip(packs, outs):
        scores = nt(pack[0], keys) * HD ** (-0.5)
        shifted = jnp.exp(scores - jnp.max(scores, axis=-1, keepdims=True))
        chances = shifted / jnp.sum(shifted, axis=-1, keepdims=True)
        out[...] = nn(chances.astype(BF), values).astype(BF)


def attention_forward(packs):
    blocks = len(packs)
    _, tokens, width = packs[0].shape
    heads = width // HD
    return pl.pallas_call(
        functools.partial(forward_body, blocks),
        grid=(heads,),
        in_specs=[pl.BlockSpec((3, tokens, HD), lambda h: (0, 0, h))] * blocks,
        out_specs=[pl.BlockSpec((tokens, HD), lambda h: (0, h))] * blocks,
        out_shape=[jax.ShapeDtypeStruct((tokens, width), BF)] * blocks,
        cost_estimate=pl.CostEstimate(
            flops=4 * heads * (blocks * tokens) ** 2 * HD,
            bytes_accessed=8 * blocks * tokens * width,
            transcendentals=heads * (blocks * tokens) ** 2,
        ),
        name="attend",
    )(*packs)


def backward_body(blocks, *refs):
    packs, grads, outs = refs[:blocks], refs[blocks : 2 * blocks], refs[2 * blocks :]
    keys = jnp.concatenate([p[1] for p in packs], axis=0)
    values = jnp.concatenate([p[2] for p in packs], axis=0)
    grad_keys = grad_values = None
    for pack, grad, out in zip(packs, grads, outs):
        query, grad_rows = pack[0], grad[...]
        scores = nt(keys, query) * HD ** (-0.5)
        shifted = jnp.exp(scores - jnp.max(scores, axis=0, keepdims=True))
        chances = shifted / jnp.sum(shifted, axis=0, keepdims=True)
        grad_chances = nt(values, grad_rows)
        add_values = nn(chances.astype(BF), grad_rows)
        inner = jnp.sum(grad_chances * chances, axis=0, keepdims=True)
        grad_scores = (chances * (grad_chances - inner) * HD ** (-0.5)).astype(BF)
        out[0] = tn(grad_scores, keys).astype(BF)
        add_keys = nn(grad_scores, query)
        grad_keys = add_keys if grad_keys is None else grad_keys + add_keys
        grad_values = add_values if grad_values is None else grad_values + add_values
    tokens = packs[0].shape[1]
    for place, out in enumerate(outs):
        out[1] = grad_keys[place * tokens : (place + 1) * tokens].astype(BF)
        out[2] = grad_values[place * tokens : (place + 1) * tokens].astype(BF)


def attention_backward(packs, grads):
    blocks = len(packs)
    _, tokens, width = packs[0].shape
    heads = width // HD
    pack_spec = pl.BlockSpec((3, tokens, HD), lambda h: (0, 0, h))
    row_spec = pl.BlockSpec((tokens, HD), lambda h: (0, h))
    return pl.pallas_call(
        functools.partial(backward_body, blocks),
        grid=(heads,),
        in_specs=[pack_spec] * blocks + [row_spec] * blocks,
        out_specs=[pack_spec] * blocks,
        out_shape=[jax.ShapeDtypeStruct((3, tokens, width), BF)] * blocks,
        cost_estimate=pl.CostEstimate(
            flops=10 * heads * (blocks * tokens) ** 2 * HD,
            bytes_accessed=14 * blocks * tokens * width,
            transcendentals=heads * (blocks * tokens) ** 2,
        ),
        name="attend_back",
    )(*packs, *grads)


class Links:
    def __init__(self):
        self.dp, self.seq = lax.axis_size("dp"), lax.axis_size("seq")
        self.pair = 2 if self.seq % 2 == 0 else 1
        self.chips = self.seq // self.pair
        self.d, self.s = lax.axis_index("dp"), lax.axis_index("seq")
        self.core = self.s % self.pair
        half = self.dp // 2
        if self.dp % 2:
            self.order = list(range(self.dp))
            self.position = self.d
        else:
            self.order = [2 * i for i in range(half)] + [2 * i + 1 for i in reversed(range(half))]
            self.position = jnp.where(self.d % 2 == 0, self.d // 2, self.dp - 1 - self.d // 2)

    def device_at(self, position):
        position = position % self.dp
        if self.dp % 2:
            return position
        return jnp.where(position < self.dp // 2, 2 * position, 2 * (self.dp - 1 - position) + 1)

    def permute(self, array, dp_to, seq_to):
        pairs = []
        for d in range(self.dp):
            for s in range(self.seq):
                pairs.append((d * self.seq + s, dp_to(d) * self.seq + seq_to(s)))
        return lax.ppermute(array, ("dp", "seq"), pairs)

    def ring(self, array, step):
        place = {d: i for i, d in enumerate(self.order)}
        return self.permute(
            array, lambda d: self.order[(place[d] + step) % self.dp], lambda s: s
        )

    def peer(self, s, k):
        chip, core = s // self.pair, s % self.pair
        return (chip + k // self.pair) % self.chips * self.pair + (core + k % self.pair) % self.pair

    def source(self, s, k):
        chip, core = s // self.pair, s % self.pair
        return (chip - k // self.pair) % self.chips * self.pair + (core - k % self.pair) % self.pair

    def out(self, array, k):
        return self.permute(array, lambda d: d, lambda s: self.peer(s, k))

    def back(self, array, k):
        return self.permute(array, lambda d: d, lambda s: self.source(s, k))

    def swap(self, array):
        return self.out(array, 1) if self.pair == 2 else array


def gather_ring(links, piece, forward):
    found = {0: piece}
    ahead, behind = piece, piece
    for step in range(1, max(forward, links.dp - 1 - forward) + 1):
        if step <= forward:
            ahead = links.ring(ahead, 1)
            found[step] = ahead
        if step <= links.dp - 1 - forward:
            behind = links.ring(behind, -1)
            found[links.dp - step] = behind
    return [found[r] for r in range(links.dp)]


def reduce_ring(links, block_of, forward):
    backward = links.dp - 1 - forward
    ahead = behind = None
    for step in range(max(forward, backward)):
        if step < forward:
            block = block_of(forward - step)
            ahead = links.ring(block if ahead is None else (ahead.astype(F32) + block.astype(F32)).astype(BF), 1)
        if step < backward:
            block = block_of(links.dp - (backward - step))
            behind = links.ring(block if behind is None else (behind.astype(F32) + block.astype(F32)).astype(BF), -1)
    total = block_of(0).astype(F32)
    for part in (ahead, behind):
        if part is not None:
            total = total + part.astype(F32)
    return total


def shards(
    queries,
    key_states,
    value_states,
    residual,
    enc_hidden,
    enc_gain,
    enc_bias,
    feature_target,
    timestep,
    gate_weight,
    lift_weight,
    out_weight,
):
    links = Links()
    n_dp, n_seq, pair = links.dp, links.seq, links.pair
    tokens, feat = queries.shape[1:]
    z_width = enc_hidden.shape[2]
    width = feat // n_seq
    gate_rows, lift_rows, out_rows = (
        gate_weight.shape[0] // pair,
        lift_weight.shape[0] // pair,
        out_weight.shape[0] // pair,
    )
    temb, hidden_units = gate_weight.shape[0] * n_dp, lift_weight.shape[1]

    def my_half(weight, core):
        rows = weight.shape[0] // pair
        return lax.dynamic_slice_in_dim(weight, core * rows, rows, 0)

    def columns(array, owner):
        return lax.dynamic_slice_in_dim(array, owner * width, width, 1)

    def pack(arrays, owner):
        return jnp.stack([columns(a, owner) for a in arrays])

    order = sorted(range(1, n_seq), key=lambda k: (k < pair, k))
    triple = (queries[0], key_states[0], value_states[0])
    packs = [pack(triple, links.s)] + [None] * (n_seq - 1)
    for k in order:
        packs[k] = links.out(pack(triple, links.peer(links.s, k)), k)

    strips = lift_rows // gate_rows
    gate_half = my_half(gate_weight, links.core)
    gate_strip = jnp.concatenate(jnp.split(gate_half, strips, axis=1), axis=0)
    first = jnp.concatenate([my_half(lift_weight, links.core), gate_strip], axis=1)
    second = my_half(out_weight, links.core)
    ahead = n_dp // 2
    first_parts = gather_ring(links, first, ahead)
    second_parts = gather_ring(links, second, n_dp - 1 - ahead)

    rows_here = jnp.concatenate(
        [
            enc_hidden[0],
            jnp.pad(
                jnp.stack([feature_target[0] // 256, feature_target[0] % 256], axis=1).astype(BF),
                ((0, 0), (0, HD - 2)),
            ),
        ],
        axis=1,
    )
    same_core = [rows_here] + [links.out(rows_here, j * pair) for j in range(1, links.chips)]
    rows_mine = jnp.concatenate(same_core, axis=0)
    rows_all = (
        jnp.concatenate([rows_mine, links.swap(rows_mine)], axis=0) if pair == 2 else rows_mine
    )
    target = (
        rows_all[:, z_width].astype(jnp.int32) * 256 + rows_all[:, z_width + 1].astype(jnp.int32)
    )
    here = links.s * tokens + jnp.arange(tokens)
    chosen = (here[:, None] == target[None, :]).astype(BF)
    picked = jnp.dot(chosen, rows_all[:, :z_width], preferred_element_type=F32)
    centred = picked - jnp.mean(picked, axis=-1, keepdims=True)
    variance = jnp.mean(centred * centred, axis=-1, keepdims=True)
    aligned = (centred * lax.rsqrt(variance + EPSILON) * enc_gain + enc_bias).astype(BF)

    def whole(parts):
        mine = jnp.stack(parts)
        other = links.swap(mine)
        rows, cols = parts[0].shape
        full = jnp.zeros((n_dp, pair, rows, cols), BF)
        for r in range(n_dp):
            source = links.device_at(links.position - r)
            full = lax.dynamic_update_slice(full, mine[r][None, None], (source, links.core, 0, 0))
            if pair == 2:
                full = lax.dynamic_update_slice(
                    full, other[r][None, None], (source, 1 - links.core, 0, 0)
                )
        return full.reshape(n_dp * pair * rows, cols)

    first_full = whole(first_parts)
    lift_full = first_full[:, :hidden_units]
    gate_full = (
        first_full[:, hidden_units:]
        .reshape(n_dp * pair, strips, gate_rows, feat // strips)
        .transpose(0, 2, 1, 3)
        .reshape(temb, feat)
    )
    out_full = whole(second_parts)

    embedded = embed_time(timestep, temb)
    gating = jnp.dot(embedded, gate_full, preferred_element_type=F32)

    mixed_parts = attention_forward(packs)
    mixed = jnp.zeros((tokens, feat), BF)
    for k in [0] + order:
        piece = mixed_parts[k] if k == 0 else links.back(mixed_parts[k], k)
        mixed = lax.dynamic_update_slice(mixed, piece, (0, links.peer(links.s, k) * width))

    mixed_wide = mixed.astype(F32)
    hidden = (residual[0].astype(F32) + gating * mixed_wide).astype(BF)
    lifted = jnp.dot(hidden, lift_full, preferred_element_type=F32)
    sigmoid_lift = jax.nn.sigmoid(lifted)
    activated = (lifted * sigmoid_lift).astype(BF)
    predicted = jnp.dot(activated, out_full, preferred_element_type=F32)
    target_wide = aligned.astype(F32)
    pred_norm = jnp.sqrt(jnp.sum(predicted * predicted, axis=1, keepdims=True) + EPSILON)
    target_norm = jnp.sqrt(jnp.sum(target_wide * target_wide, axis=1, keepdims=True) + EPSILON)
    cosine = jnp.sum(predicted * target_wide, axis=1, keepdims=True) / (pred_norm * target_norm)
    grad_pred = (
        -1.0
        * z_width
        * (target_wide / (pred_norm * target_norm) - cosine * predicted / (pred_norm * pred_norm))
    ).astype(BF)
    grad_act = jnp.einsum("tz,pz->tp", grad_pred, out_full, preferred_element_type=F32)
    grad_lifted = (grad_act * sigmoid_lift * (1.0 + lifted * (1.0 - sigmoid_lift))).astype(BF)
    grad_hidden = jnp.einsum("tp,fp->tf", grad_lifted, lift_full, preferred_element_type=F32)
    grad_mixed = (gating * grad_hidden).astype(BF)
    grad_gating = jnp.sum(grad_hidden * mixed_wide, axis=0, keepdims=True)

    grads = [columns(grad_mixed, links.s)] + [None] * (n_seq - 1)
    for k in order:
        grads[k] = links.out(columns(grad_mixed, links.peer(links.s, k)), k)

    def half_columns(array, core):
        split = array.reshape(tokens, n_dp, pair, -1)
        return lax.dynamic_slice_in_dim(split, core, 1, 2).reshape(tokens, -1)

    hidden_mine, act_mine = half_columns(hidden, links.core), half_columns(activated, links.core)
    left = [hidden_mine, grad_lifted, act_mine, grad_pred]
    if pair == 2:
        sent = jnp.concatenate(
            [
                half_columns(hidden, 1 - links.core),
                grad_lifted,
                half_columns(activated, 1 - links.core),
                grad_pred,
            ],
            axis=1,
        )
        cuts = [sum(a.shape[1] for a in left[: i + 1]) for i in range(3)]
        left = [
            jnp.concatenate([a, b], axis=0)
            for a, b in zip(left, jnp.split(links.swap(sent), cuts, axis=1))
        ]
        grad_gating = grad_gating + links.swap(grad_gating)
    part_lift = jnp.einsum("tf,tp->fp", left[0], left[1], preferred_element_type=F32).astype(BF)
    part_out = jnp.einsum("tp,tz->pz", left[2], left[3], preferred_element_type=F32).astype(BF)
    part_lift = part_lift.reshape(n_dp, lift_rows, hidden_units)
    part_out = part_out.reshape(n_dp, out_rows, z_width)
    wide_embedded = embedded.astype(F32).reshape(n_dp, pair, gate_rows)
    strips_grad = grad_gating.reshape(strips, 1, feat // strips)

    def block_first(r):
        target_device = links.device_at(links.position + r)
        block = lax.dynamic_index_in_dim(part_lift, target_device, 0, False)
        ours = lax.dynamic_slice(wide_embedded, (target_device, links.core, 0), (1, 1, gate_rows))
        gate = (ours.reshape(1, gate_rows, 1) * strips_grad).reshape(lift_rows, feat // strips)
        return jnp.concatenate([block, gate.astype(BF)], axis=1)

    def block_second(r):
        return lax.dynamic_index_in_dim(part_out, links.device_at(links.position + r), 0, False)

    share_second = reduce_ring(links, block_second, n_dp - 1 - ahead).astype(BF)
    share_first = reduce_ring(links, block_first, ahead).astype(BF)

    def over_seq(share):
        total = share.astype(F32)
        for j in range(1, links.chips):
            total = total + links.out(share, j * pair).astype(F32)
        if pair == 1:
            return total
        mine = total.astype(BF)
        other = links.swap(mine)
        lower = jnp.where(links.core == 0, mine, other)
        upper = jnp.where(links.core == 0, other, mine)
        return jnp.stack([lower, upper]).astype(F32)

    second_sum = over_seq(share_second)
    first_sum = over_seq(share_first).reshape(pair, lift_rows, -1)
    grad_out = second_sum.reshape(pair * out_rows, z_width)
    grad_lift = first_sum[:, :, :hidden_units].reshape(pair * lift_rows, hidden_units)
    grad_gate = (
        first_sum[:, :, hidden_units:]
        .reshape(pair, strips, gate_rows, feat // strips)
        .transpose(0, 2, 1, 3)
        .reshape(pair * gate_rows, feat)
    )

    back = attention_backward(packs, grads)
    done = [jnp.zeros((tokens, feat), BF) for _ in range(3)]
    for k in [0] + order:
        piece = back[k] if k == 0 else links.back(back[k], k)
        place = links.peer(links.s, k) * width
        done = [lax.dynamic_update_slice(a, piece[i], (0, place)) for i, a in enumerate(done)]
    return (done[0][None], done[1][None], done[2][None], grad_gate, grad_lift, grad_out)


def solution(mesh):
    in_specs = (
        P("dp", "seq", None),
        P("dp", "seq", None),
        P("dp", "seq", None),
        P("dp", "seq", None),
        P("dp", "seq", None),
        P(),
        P(),
        P("dp", "seq"),
        P("dp"),
        P("dp", None),
        P("dp", None),
        P("dp", None),
    )
    out_specs = (
        P("dp", "seq", None),
        P("dp", "seq", None),
        P("dp", "seq", None),
        P("dp", None),
        P("dp", None),
        P("dp", None),
    )
    return jax.shard_map(shards, mesh=mesh, in_specs=in_specs, out_specs=out_specs, check_vma=False)
```

```python
import functools
import math

import jax
import jax.numpy as jnp
from jax import lax
from jax.experimental import pallas as pl
from jax.experimental.pallas import tpu as pltpu
from jax.sharding import PartitionSpec as P

HD = 128
EPSILON = 1e-06
BF = jnp.bfloat16
F32 = jnp.float32


def embed_time(timestep, width):
    half_width = width // 2
    frequency = jnp.exp(
        -math.log(10000.0) * jnp.arange(half_width).astype(F32) / half_width
    )
    angles = timestep.astype(F32)[:, None] * frequency[None, :]
    return jnp.concatenate([jnp.cos(angles), jnp.sin(angles)], axis=1).astype(BF)


def nt(a, b):
    return lax.dot_general(a, b, (((1,), (1,)), ((), ())), preferred_element_type=F32)


def nn(a, b):
    return lax.dot_general(a, b, (((1,), (0,)), ((), ())), preferred_element_type=F32)


def tn(a, b):
    return lax.dot_general(a, b, (((0,), (0,)), ((), ())), preferred_element_type=F32)


def forward_body(blocks, *refs):
    packs, outs = refs[:blocks], refs[blocks:]
    keys = jnp.concatenate([p[1] for p in packs], axis=0)
    values = jnp.concatenate([p[2] for p in packs], axis=0)
    for pack, out in zip(packs, outs):
        scores = nt(pack[0], keys) * HD ** (-0.5)
        shifted = jnp.exp(scores - jnp.max(scores, axis=-1, keepdims=True))
        chances = shifted / jnp.sum(shifted, axis=-1, keepdims=True)
        out[...] = nn(chances.astype(BF), values).astype(BF)


def attention_forward(packs):
    blocks = len(packs)
    _, tokens, width = packs[0].shape
    heads = width // HD
    return pl.pallas_call(
        functools.partial(forward_body, blocks),
        grid=(heads,),
        in_specs=[pl.BlockSpec((3, tokens, HD), lambda h: (0, 0, h))] * blocks,
        out_specs=[pl.BlockSpec((tokens, HD), lambda h: (0, h))] * blocks,
        out_shape=[jax.ShapeDtypeStruct((tokens, width), BF)] * blocks,
        cost_estimate=pl.CostEstimate(
            flops=4 * heads * (blocks * tokens) ** 2 * HD,
            bytes_accessed=8 * blocks * tokens * width,
            transcendentals=heads * (blocks * tokens) ** 2,
        ),
        name="attend",
    )(*packs)


def backward_body(blocks, *refs):
    packs, grads, outs = refs[:blocks], refs[blocks : 2 * blocks], refs[2 * blocks + 1 :]
    keys = jnp.concatenate([p[1] for p in packs], axis=0)
    values = jnp.concatenate([p[2] for p in packs], axis=0)
    grad_keys = grad_values = None
    for pack, grad, out in zip(packs, grads, outs):
        query, grad_rows = pack[0], grad[...]
        scores = nt(keys, query) * HD ** (-0.5)
        shifted = jnp.exp(scores - jnp.max(scores, axis=0, keepdims=True))
        chances = shifted / jnp.sum(shifted, axis=0, keepdims=True)
        grad_chances = nt(values, grad_rows)
        add_values = nn(chances.astype(BF), grad_rows)
        inner = jnp.sum(grad_chances * chances, axis=0, keepdims=True)
        grad_scores = (chances * (grad_chances - inner) * HD ** (-0.5)).astype(BF)
        out[0] = tn(grad_scores, keys).astype(BF)
        add_keys = nn(grad_scores, query)
        grad_keys = add_keys if grad_keys is None else grad_keys + add_keys
        grad_values = add_values if grad_values is None else grad_values + add_values
    tokens = packs[0].shape[1]
    for place, out in enumerate(outs):
        out[1] = grad_keys[place * tokens : (place + 1) * tokens].astype(BF)
        out[2] = grad_values[place * tokens : (place + 1) * tokens].astype(BF)


def attention_backward(packs, grads, after):
    blocks = len(packs)
    _, tokens, width = packs[0].shape
    heads = width // HD
    pack_spec = pl.BlockSpec((3, tokens, HD), lambda h: (0, 0, h))
    row_spec = pl.BlockSpec((tokens, HD), lambda h: (0, h))
    return pl.pallas_call(
        functools.partial(backward_body, blocks),
        grid=(heads,),
        in_specs=[pack_spec] * blocks + [row_spec] * blocks + [pl.BlockSpec(memory_space=pl.ANY)],
        out_specs=[pack_spec] * blocks,
        out_shape=[jax.ShapeDtypeStruct((3, tokens, width), BF)] * blocks,
        cost_estimate=pl.CostEstimate(
            flops=10 * heads * (blocks * tokens) ** 2 * HD,
            bytes_accessed=14 * blocks * tokens * width,
            transcendentals=heads * (blocks * tokens) ** 2,
        ),
        name="attend_back",
    )(*packs, *grads, after)


class Links:
    def __init__(self):
        self.dp, self.seq = lax.axis_size("dp"), lax.axis_size("seq")
        self.pair = 2 if self.seq % 2 == 0 else 1
        self.chips = self.seq // self.pair
        self.d, self.s = lax.axis_index("dp"), lax.axis_index("seq")
        self.core = self.s % self.pair
        half = self.dp // 2
        if self.dp % 2:
            self.order = list(range(self.dp))
            self.position = self.d
        else:
            self.order = [2 * i for i in range(half)] + [2 * i + 1 for i in reversed(range(half))]
            self.position = jnp.where(self.d % 2 == 0, self.d // 2, self.dp - 1 - self.d // 2)

    def device_at(self, position):
        position = position % self.dp
        if self.dp % 2:
            return position
        return jnp.where(position < self.dp // 2, 2 * position, 2 * (self.dp - 1 - position) + 1)

    def permute(self, array, dp_to, seq_to):
        pairs = []
        for d in range(self.dp):
            for s in range(self.seq):
                pairs.append((d * self.seq + s, dp_to(d) * self.seq + seq_to(s)))
        return lax.ppermute(array, ("dp", "seq"), pairs)

    def ring(self, array, step):
        place = {d: i for i, d in enumerate(self.order)}
        return self.permute(
            array, lambda d: self.order[(place[d] + step) % self.dp], lambda s: s
        )

    def peer(self, s, k):
        chip, core = s // self.pair, s % self.pair
        return (chip + k // self.pair) % self.chips * self.pair + (core + k % self.pair) % self.pair

    def source(self, s, k):
        chip, core = s // self.pair, s % self.pair
        return (chip - k // self.pair) % self.chips * self.pair + (core - k % self.pair) % self.pair

    def out(self, array, k):
        return self.permute(array, lambda d: d, lambda s: self.peer(s, k))

    def back(self, array, k):
        return self.permute(array, lambda d: d, lambda s: self.source(s, k))

    def swap(self, array):
        return self.out(array, 1) if self.pair == 2 else array


def gather_ring(links, piece, forward):
    found = {0: piece}
    ahead, behind = piece, piece
    for step in range(1, max(forward, links.dp - 1 - forward) + 1):
        if step <= forward:
            ahead = links.ring(ahead, 1)
            found[step] = ahead
        if step <= links.dp - 1 - forward:
            behind = links.ring(behind, -1)
            found[links.dp - step] = behind
    return [found[r] for r in range(links.dp)]


def plus(a, b):
    return (a.astype(F32) + b.astype(F32)).astype(BF)


def reduce_ring(links, blocks, forward):
    backward = links.dp - 1 - forward
    ahead = behind = None
    for step in range(max(forward, backward)):
        if step < forward:
            block = blocks[forward - step]
            ahead = links.ring(block if ahead is None else plus(ahead, block), 1)
        if step < backward:
            block = blocks[links.dp - (backward - step)]
            behind = links.ring(block if behind is None else plus(behind, block), -1)
    total = blocks[0].astype(F32)
    for part in (ahead, behind):
        if part is not None:
            total = total + part.astype(F32)
    return total


VMEM_SPEC = pl.BlockSpec(memory_space=pltpu.VMEM)
SMEM_SPEC = pl.BlockSpec(memory_space=pltpu.SMEM)
ANY_SPEC = pl.BlockSpec(memory_space=pl.ANY)


def at(start, size):
    return pl.ds(pl.multiple_of(start, HD), size)


def call(body, name, operands, specs, shapes, scratch=(), flops=0):
    moved = sum(a.size * a.dtype.itemsize for a in operands)
    moved += sum(math.prod(a.shape) * a.dtype.itemsize for a in shapes)
    return pl.pallas_call(
        body,
        in_specs=specs,
        out_specs=[VMEM_SPEC] * len(shapes),
        out_shape=shapes,
        scratch_shapes=list(scratch),
        cost_estimate=pl.CostEstimate(flops=flops + moved, bytes_accessed=moved, transcendentals=0),
        compiler_params=pltpu.CompilerParams(vmem_limit_bytes=58 * 1024 * 1024),
        name=name,
    )(*operands)


def cut_weights(core, lift, out, gate, pair):
    rows, units = lift.shape
    gate_rows, feat = gate.shape
    strips, part = rows // gate_rows, units // pair
    strip = feat // pair // strips
    z_part = out.shape[1] // pair

    def body(core_ref, lift_ref, out_ref, gate_ref, *outs):
        for j in range(pair):
            c = (core_ref[0] + j) % pair
            first, second = outs[2 * j], outs[2 * j + 1]
            first[:, :part] = lift_ref[:, at(c * part, part)]
            for q in range(strips):
                first[q * gate_rows : (q + 1) * gate_rows, part:] = gate_ref[
                    :, at((c * strips + q) * strip, strip)
                ]
            second[...] = out_ref[:, at(c * z_part, z_part)]

    shapes = [
        jax.ShapeDtypeStruct((rows, part + strip), BF),
        jax.ShapeDtypeStruct((out.shape[0], z_part), BF),
    ] * pair
    return call(
        body, "cut", (core, lift, out, gate), [SMEM_SPEC] + [VMEM_SPEC] * 3, shapes
    )


def pack_inputs(owners, queries, keys, values, encoder, target, width):
    tokens, z_width = encoder.shape
    n_seq = queries.shape[1] // width

    def body(owner_ref, q_ref, k_ref, v_ref, e_ref, t_ref, *outs):
        for k in range(n_seq):
            for i, ref in enumerate((q_ref, k_ref, v_ref)):
                outs[k][i] = ref[:, at(owner_ref[k] * width, width)]
        rows = outs[n_seq]
        rows[:, :z_width] = e_ref[...]
        line = lax.broadcasted_iota(jnp.int32, (tokens, tokens), 0)
        lane = lax.broadcasted_iota(jnp.int32, (tokens, tokens), 1)
        place = jnp.sum(
            jnp.where(line == lane, jnp.broadcast_to(t_ref[...], (tokens, tokens)), 0).astype(F32),
            axis=1,
            keepdims=True,
        )
        high = jnp.floor(place * (1.0 / 256.0))
        low = place - 256.0 * high
        side = lax.broadcasted_iota(jnp.int32, (tokens, HD), 1)
        rows[:, z_width:] = jnp.where(side == 0, high, jnp.where(side == 1, low, 0.0)).astype(BF)

    shapes = [jax.ShapeDtypeStruct((3, tokens, width), BF)] * n_seq
    shapes.append(jax.ShapeDtypeStruct((tokens, z_width + HD), BF))
    return call(
        body,
        "pack",
        (owners, queries, keys, values, encoder, target),
        [SMEM_SPEC] + [VMEM_SPEC] * 5,
        shapes,
    )


def align_features(first_token, rows, tokens, gain, bias):
    z_width = gain.shape[1]

    def body(token_ref, gain_ref, bias_ref, *refs):
        out = refs[-1]
        picked = None
        for ref in refs[:-1]:
            count = ref.shape[0]
            place = ref[:, z_width:].astype(F32)
            target = place[:, 0:1] * 256.0 + place[:, 1:2]
            here = lax.broadcasted_iota(jnp.int32, (count, tokens), 1) + token_ref[0]
            chosen = jnp.where(target == here.astype(F32), 1.0, 0.0).astype(BF)
            part = tn(chosen, ref[:, :z_width])
            picked = part if picked is None else picked + part
        centred = picked - jnp.mean(picked, axis=-1, keepdims=True)
        variance = jnp.mean(centred * centred, axis=-1, keepdims=True)
        out[...] = (
            centred * lax.rsqrt(variance + EPSILON) * gain_ref[...] + bias_ref[...]
        ).astype(BF)

    return call(
        body,
        "align",
        (first_token, gain, bias, *rows),
        [SMEM_SPEC] + [VMEM_SPEC] * (2 + len(rows)),
        [jax.ShapeDtypeStruct((tokens, z_width), BF)],
        flops=2 * tokens * sum(r.shape[0] for r in rows) * z_width,
    )[0]


def project(index, spread, residual, aligned, mixed, firsts, seconds, sizes):
    n_dp, n_seq, pair, units, strips = sizes
    tokens, feat = residual.shape
    z_width = aligned.shape[1]
    width = feat // n_seq
    rows, first_cols = firsts[0][0].shape
    part, strip = units // pair, first_cols - units // pair
    out_rows, z_part = seconds[0][0].shape
    n_pieces = n_dp * pair

    def body(index_ref, spread_ref, residual_ref, aligned_ref, *refs):
        refs = list(refs)
        take = lambda n: [refs.pop(0) for _ in range(n)]
        mixed_refs, first_refs, second_refs = take(n_seq), take(n_pieces), take(n_pieces)
        sent, kept, grad_gating = take(3)
        grad_pieces = take(n_seq)
        lift, out, gate, gating, hidden, grad_hidden, sems = refs
        core = index_ref[0]

        copies = []
        for r in range(n_dp):
            d = index_ref[1 + n_seq + r]
            for j in range(pair):
                c = (core + j) % pair
                i = r * pair + j
                copies.append(
                    (
                        pltpu.make_async_copy(
                            first_refs[i].at[:, pl.ds(part, strip)],
                            gate.at[c, pl.ds(pl.multiple_of(d * rows, rows), rows), :],
                            sems.at[0, i],
                        ),
                        pltpu.make_async_copy(
                            first_refs[i].at[:, pl.ds(0, part)],
                            lift.at[pl.ds(pl.multiple_of(d * rows, rows), rows), at(c * part, part)],
                            sems.at[1, i],
                        ),
                        pltpu.make_async_copy(
                            second_refs[i],
                            out.at[
                                pl.ds(pl.multiple_of(d * out_rows, out_rows), out_rows),
                                at(c * z_part, z_part),
                            ],
                            sems.at[2, i],
                        ),
                    )
                )
        for kind in range(3):
            for copy in copies:
                copy[kind].start()
        for copy in copies:
            copy[0].wait()
        for c in range(pair):
            lines = nn(spread_ref[...], gate[c])
            for q in range(strips):
                start = (c * strips + q) * strip
                gating[:, start : start + strip] = lines[q : q + 1, :]
        for k in range(n_seq):
            here = at(index_ref[1 + k] * width, width)
            hidden[:, here] = (
                residual_ref[:, here].astype(F32) + gating[:, here] * mixed_refs[k][...].astype(F32)
            ).astype(BF)
        for copy in copies:
            copy[1].wait()
        lifted = nn(hidden[...], lift[...])
        sigmoid = 1.0 / (1.0 + jnp.exp(-lifted))
        activated = (lifted * sigmoid).astype(BF)
        slope = sigmoid * (1.0 + lifted * (1.0 - sigmoid))
        for copy in copies:
            copy[2].wait()
        predicted = nn(activated, out[...])
        target = aligned_ref[...].astype(F32)
        pred_norm = jnp.sqrt(jnp.sum(predicted * predicted, axis=1, keepdims=True) + EPSILON)
        target_norm = jnp.sqrt(jnp.sum(target * target, axis=1, keepdims=True) + EPSILON)
        cosine = jnp.sum(predicted * target, axis=1, keepdims=True) / (pred_norm * target_norm)
        scale = -1.0 * z_width / (pred_norm * target_norm)
        pull = z_width * cosine / (pred_norm * pred_norm)
        grad_pred = (scale * target + pull * predicted).astype(BF)
        grad_lifted = (nt(grad_pred, out[...]) * slope).astype(BF)
        sent[:, :feat] = hidden[...]
        sent[:, feat : feat + units] = activated
        grad_hidden[...] = nt(grad_lifted, lift[...])
        lift[:tokens, :units] = grad_lifted
        out[:tokens, :z_width] = grad_pred
        other = (core + pair - 1) % pair
        sent[:, feat + units : feat + units + part] = lift[:tokens, at(other * part, part)]
        sent[:, feat + units + part :] = out[:tokens, at(other * z_part, z_part)]
        kept[:, :part] = lift[:tokens, at(core * part, part)]
        kept[:, part:] = out[:tokens, at(core * z_part, z_part)]
        for k in range(n_seq):
            here = at(index_ref[1 + k] * width, width)
            grads = grad_hidden[:, here]
            grad_pieces[k][...] = (gating[:, here] * grads).astype(BF)
            grad_gating[:, here] = jnp.sum(
                grads * mixed_refs[k][...].astype(F32), axis=0, keepdims=True
            )

    shapes = [
        jax.ShapeDtypeStruct((tokens, feat + units + part + z_part), BF),
        jax.ShapeDtypeStruct((tokens, part + z_part), BF),
        jax.ShapeDtypeStruct((1, feat), F32),
    ] + [jax.ShapeDtypeStruct((tokens, width), BF)] * n_seq
    flat = lambda pieces: [p for both in pieces for p in both]
    return call(
        body,
        "project",
        (index, spread, residual, aligned, *mixed, *flat(firsts), *flat(seconds)),
        [SMEM_SPEC] + [VMEM_SPEC] * (3 + n_seq) + [ANY_SPEC] * (2 * n_pieces),
        shapes,
        [
            pltpu.VMEM((n_dp * rows, units), BF),
            pltpu.VMEM((n_dp * out_rows, z_width), BF),
            pltpu.VMEM((pair, n_dp * rows, strip), BF),
            pltpu.VMEM((1, feat), F32),
            pltpu.VMEM((tokens, feat), BF),
            pltpu.VMEM((tokens, feat), F32),
            pltpu.SemaphoreType.DMA((3, n_pieces)),
        ],
        flops=6 * tokens * units * (feat + z_width),
    )


def out_blocks(index, sent, got, kept, sizes, z_part, out_rows):
    n_dp, n_seq, pair, units, _ = sizes
    tokens, cols = sent.shape
    act = cols - units - units // pair - z_part
    halves = [sent] if got is None else [sent, got]

    def body(index_ref, kept_ref, *refs):
        sources, outs = refs[: len(halves)], refs[len(halves) :]
        grads = [kept_ref[:, units // pair :]]
        if got is not None:
            grads.append(sources[1][:, cols - z_part :])
        grads = jnp.concatenate(grads, axis=0)
        for r in range(n_dp):
            here = at(act + index_ref[1 + n_seq + n_dp + r] * out_rows, out_rows)
            left = jnp.concatenate([s[:, here] for s in sources], axis=0)
            outs[r][...] = tn(left, grads).astype(BF)

    return call(
        body,
        "grad_out",
        (index, kept, *halves),
        [SMEM_SPEC] + [VMEM_SPEC] * (1 + len(halves)),
        [jax.ShapeDtypeStruct((out_rows, z_part), BF)] * n_dp,
        flops=4 * tokens * z_part * units,
    )


def lift_blocks(index, sent, got, kept, grad_gating, embedded, sizes, rows, strip):
    n_dp, n_seq, pair, units, strips = sizes
    tokens, feat = sent.shape[0], n_dp * rows
    part, gate_rows = units // pair, rows // strips
    halves = [sent] if got is None else [sent, got]
    sums = len(grad_gating)

    def body(index_ref, kept_ref, embedded_ref, *refs):
        gating_refs, sources, outs = refs[:sums], refs[sums : sums + len(halves)], refs[sums + len(halves) :]
        grads = [kept_ref[:, :part]]
        if got is not None:
            grads.append(sources[1][:, feat + units : feat + units + part])
        grads = jnp.concatenate(grads, axis=0)
        core = index_ref[0]
        for r in range(n_dp):
            d = index_ref[1 + n_seq + n_dp + r]
            here = at(d * rows, rows)
            left = jnp.concatenate([s[:, here] for s in sources], axis=0)
            outs[r][:, :part] = tn(left, grads).astype(BF)
            line = embedded_ref[pl.ds(pl.multiple_of(d * gate_rows, gate_rows), gate_rows), :]
            for q in range(strips):
                there = at((core * strips + q) * strip, strip)
                gate = sum(g[:, there] for g in gating_refs)
                outs[r][q * gate_rows : (q + 1) * gate_rows, part:] = (line * gate).astype(BF)

    return call(
        body,
        "grad_lift",
        (index, kept, embedded, *grad_gating, *halves),
        [SMEM_SPEC] + [VMEM_SPEC] * (2 + sums + len(halves)),
        [jax.ShapeDtypeStruct((rows, part + strip), BF)] * n_dp,
        flops=4 * tokens * part * feat,
    )


def place_shares(core, firsts, seconds, sizes):
    _, _, pair, units, strips = sizes
    rows, cols = firsts[0].shape
    part, strip = units // pair, cols - units // pair
    gate_rows = rows // strips
    out_rows, z_part = seconds[0].shape

    def body(core_ref, *refs):
        first_refs, second_refs = refs[:pair], refs[pair : 2 * pair]
        gate, lift, out = refs[2 * pair :]
        for j in range(pair):
            c = (core_ref[0] + j) % pair
            lift[:, at(c * part, part)] = first_refs[j][:, :part].astype(F32)
            out[:, at(c * z_part, z_part)] = second_refs[j][...].astype(F32)
            for q in range(strips):
                gate[:, at((c * strips + q) * strip, strip)] = first_refs[j][
                    q * gate_rows : (q + 1) * gate_rows, part:
                ].astype(F32)

    return call(
        body,
        "place",
        (core, *firsts, *seconds),
        [SMEM_SPEC] + [VMEM_SPEC] * (2 * pair),
        [
            jax.ShapeDtypeStruct((gate_rows, strip * strips * pair), F32),
            jax.ShapeDtypeStruct((rows, units), F32),
            jax.ShapeDtypeStruct((out_rows, z_part * pair), F32),
        ],
    )


def place_grads(owners, pieces):
    _, tokens, width = pieces[0].shape

    def body(owner_ref, *refs):
        sources, outs = refs[: len(pieces)], refs[len(pieces) :]
        for k, ref in enumerate(sources):
            for i in range(3):
                outs[i][:, at(owner_ref[k] * width, width)] = ref[i]

    return call(
        body,
        "unpack",
        (owners, *pieces),
        [SMEM_SPEC] + [VMEM_SPEC] * len(pieces),
        [jax.ShapeDtypeStruct((tokens, width * len(pieces)), BF)] * 3,
    )


def shards(
    queries,
    key_states,
    value_states,
    residual,
    enc_hidden,
    enc_gain,
    enc_bias,
    feature_target,
    timestep,
    gate_weight,
    lift_weight,
    out_weight,
):
    links = Links()
    n_dp, n_seq, pair = links.dp, links.seq, links.pair
    tokens, feat = queries.shape[1:]
    width = feat // n_seq
    rows, units = lift_weight.shape
    gate_rows = gate_weight.shape[0]
    temb, strips = gate_rows * n_dp, rows // gate_rows
    sizes = (n_dp, n_seq, pair, units, strips)
    order = sorted(range(1, n_seq), key=lambda k: (k < pair, k))
    owners = [links.peer(links.s, k) for k in range(n_seq)]
    index = jnp.stack(
        [links.core]
        + owners
        + [links.device_at(links.position - r) for r in range(n_dp)]
        + [links.device_at(links.position + r) for r in range(n_dp)]
    ).astype(jnp.int32)
    core_index = index[:1]
    owner_index = index[1 : 1 + n_seq]

    halves = cut_weights(core_index, lift_weight, out_weight, gate_weight, pair)
    ahead = n_dp // 2
    first_parts = gather_ring(links, halves[0], ahead)
    second_parts = gather_ring(links, halves[1], n_dp - 1 - ahead)

    def with_other(parts, own):
        if pair == 1:
            return [[p] for p in parts]
        return [[parts[0], own]] + [[p, links.swap(p)] for p in parts[1:]]

    firsts = with_other(first_parts, halves[2 * pair - 2])
    seconds = with_other(second_parts, halves[2 * pair - 1])

    packed = pack_inputs(
        owner_index,
        queries[0],
        key_states[0],
        value_states[0],
        enc_hidden[0],
        feature_target,
        width,
    )
    packs = [packed[0]] + [None] * (n_seq - 1)
    for k in order:
        packs[k] = links.out(packed[k], k)
    clip_rows = [packed[n_seq]]
    clip_rows += [links.out(packed[n_seq], j * pair) for j in range(1, links.chips)]
    if pair == 2:
        clip_rows += [links.swap(r) for r in clip_rows]
    aligned = align_features(
        (links.s * tokens).astype(jnp.int32)[None],
        clip_rows,
        tokens,
        enc_gain[None],
        enc_bias[None],
    )

    embedded = embed_time(timestep, temb)
    spread = (
        embedded.reshape(n_dp, 1, 1, gate_rows) * jnp.eye(strips, dtype=BF)[None, :, :, None]
    )
    spread = spread.transpose(1, 0, 2, 3).reshape(strips, n_dp * rows)
    tall = jnp.broadcast_to(embedded.astype(F32).reshape(temb, 1), (temb, feat // pair // strips))

    attended = attention_forward(packs)
    mixed = [attended[0]] + [None] * (n_seq - 1)
    for k in order:
        mixed[k] = links.back(attended[k], k)

    sent, kept, grad_gating, *pieces = project(
        index, spread, residual[0], aligned, mixed, firsts, seconds, sizes
    )
    got, gatings = None, [grad_gating]
    if pair == 2:
        got = links.swap(sent)
        gatings.append(links.swap(grad_gating))
    grads = [pieces[0]] + [None] * (n_seq - 1)
    for k in order:
        grads[k] = links.out(pieces[k], k)

    part_out = out_blocks(
        index, sent, got, kept, sizes, halves[1].shape[1], halves[1].shape[0]
    )
    part_lift = lift_blocks(
        index, sent, got, kept, gatings, tall, sizes, rows, feat // pair // strips
    )
    share_second = reduce_ring(links, part_out, n_dp - 1 - ahead)
    share_first = reduce_ring(links, part_lift, ahead)

    def over_seq(share):
        mine = share.astype(BF)
        total = share
        for j in range(1, links.chips):
            total = total + links.out(mine, j * pair).astype(F32)
        mine = total.astype(BF)
        return [mine] if pair == 1 else [mine, links.swap(mine)]

    grad_gate, grad_lift, grad_out = place_shares(
        core_index, over_seq(share_first), over_seq(share_second), sizes
    )

    back = attention_backward(packs, grads, part_lift[0])
    done = [back[0]] + [None] * (n_seq - 1)
    for k in order:
        done[k] = links.back(back[k], k)
    d_queries, d_keys, d_values = place_grads(owner_index, done)
    return (d_queries[None], d_keys[None], d_values[None], grad_gate, grad_lift, grad_out)


def solution(mesh):
    in_specs = (
        P("dp", "seq", None),
        P("dp", "seq", None),
        P("dp", "seq", None),
        P("dp", "seq", None),
        P("dp", "seq", None),
        P(),
        P(),
        P("dp", "seq"),
        P("dp"),
        P("dp", None),
        P("dp", None),
        P("dp", None),
    )
    out_specs = (
        P("dp", "seq", None),
        P("dp", "seq", None),
        P("dp", "seq", None),
        P("dp", None),
        P("dp", None),
        P("dp", None),
    )
    return jax.shard_map(shards, mesh=mesh, in_specs=in_specs, out_specs=out_specs, check_vma=False)
```

```python
import functools
import math

import jax
import jax.numpy as jnp
from jax import lax
from jax.experimental import pallas as pl
from jax.experimental.pallas import tpu as pltpu
from jax.sharding import PartitionSpec as P


HD = 128
EPSILON = 1e-06
BF = jnp.bfloat16
F32 = jnp.float32


def embed_time(timestep, width):
    half_width = width // 2
    frequency = jnp.exp(
        -math.log(10000.0) * jnp.arange(half_width).astype(F32) / half_width
    )
    angles = timestep.astype(F32)[:, None] * frequency[None, :]
    return jnp.concatenate([jnp.cos(angles), jnp.sin(angles)], axis=1).astype(BF)


def nt(a, b):
    return lax.dot_general(a, b, (((1,), (1,)), ((), ())), preferred_element_type=F32)


def nn(a, b):
    return lax.dot_general(a, b, (((1,), (0,)), ((), ())), preferred_element_type=F32)


def tn(a, b):
    return lax.dot_general(a, b, (((0,), (0,)), ((), ())), preferred_element_type=F32)


def forward_body(blocks, *refs):
    packs, outs = refs[:blocks], refs[blocks:]
    keys = jnp.concatenate([p[1] for p in packs], axis=0)
    values = jnp.concatenate([p[2] for p in packs], axis=0)
    for pack, out in zip(packs, outs):
        scores = nt(pack[0], keys) * HD ** (-0.5)
        shifted = jnp.exp(scores - jnp.max(scores, axis=-1, keepdims=True))
        chances = shifted / jnp.sum(shifted, axis=-1, keepdims=True)
        out[...] = nn(chances.astype(BF), values).astype(BF)


def attention_forward(packs):
    blocks = len(packs)
    _, tokens, width = packs[0].shape
    heads = width // HD
    return pl.pallas_call(
        functools.partial(forward_body, blocks),
        grid=(heads,),
        in_specs=[pl.BlockSpec((3, tokens, HD), lambda h: (0, 0, h))] * blocks,
        out_specs=[pl.BlockSpec((tokens, HD), lambda h: (0, h))] * blocks,
        out_shape=[jax.ShapeDtypeStruct((tokens, width), BF)] * blocks,
        cost_estimate=pl.CostEstimate(
            flops=4 * heads * (blocks * tokens) ** 2 * HD,
            bytes_accessed=8 * blocks * tokens * width,
            transcendentals=heads * (blocks * tokens) ** 2,
        ),
        name="attend",
    )(*packs)


def backward_body(blocks, *refs):
    packs, grads, outs = refs[:blocks], refs[blocks : 2 * blocks], refs[2 * blocks + 1 :]
    keys = jnp.concatenate([p[1] for p in packs], axis=0)
    values = jnp.concatenate([p[2] for p in packs], axis=0)
    grad_keys = grad_values = None
    for pack, grad, out in zip(packs, grads, outs):
        query, grad_rows = pack[0], grad[...]
        scores = nt(keys, query) * HD ** (-0.5)
        shifted = jnp.exp(scores - jnp.max(scores, axis=0, keepdims=True))
        chances = shifted / jnp.sum(shifted, axis=0, keepdims=True)
        grad_chances = nt(values, grad_rows)
        add_values = nn(chances.astype(BF), grad_rows)
        inner = jnp.sum(grad_chances * chances, axis=0, keepdims=True)
        grad_scores = (chances * (grad_chances - inner) * HD ** (-0.5)).astype(BF)
        out[0] = tn(grad_scores, keys).astype(BF)
        add_keys = nn(grad_scores, query)
        grad_keys = add_keys if grad_keys is None else grad_keys + add_keys
        grad_values = add_values if grad_values is None else grad_values + add_values
    tokens = packs[0].shape[1]
    for place, out in enumerate(outs):
        out[1] = grad_keys[place * tokens : (place + 1) * tokens].astype(BF)
        out[2] = grad_values[place * tokens : (place + 1) * tokens].astype(BF)


def attention_backward(packs, grads, after):
    blocks = len(packs)
    _, tokens, width = packs[0].shape
    heads = width // HD
    pack_spec = pl.BlockSpec((3, tokens, HD), lambda h: (0, 0, h))
    row_spec = pl.BlockSpec((tokens, HD), lambda h: (0, h))
    return pl.pallas_call(
        functools.partial(backward_body, blocks),
        grid=(heads,),
        in_specs=[pack_spec] * blocks + [row_spec] * blocks + [pl.BlockSpec(memory_space=pl.ANY)],
        out_specs=[pack_spec] * blocks,
        out_shape=[jax.ShapeDtypeStruct((3, tokens, width), BF)] * blocks,
        cost_estimate=pl.CostEstimate(
            flops=10 * heads * (blocks * tokens) ** 2 * HD,
            bytes_accessed=14 * blocks * tokens * width,
            transcendentals=heads * (blocks * tokens) ** 2,
        ),
        name="attend_back",
    )(*packs, *grads, after)


class Links:
    def __init__(self):
        self.dp, self.seq = lax.axis_size("dp"), lax.axis_size("seq")
        self.pair = 2 if self.seq % 2 == 0 else 1
        self.chips = self.seq // self.pair
        self.d, self.s = lax.axis_index("dp"), lax.axis_index("seq")
        half = self.dp // 2
        if self.dp % 2:
            self.order = list(range(self.dp))
        else:
            self.order = [2 * i for i in range(half)] + [2 * i + 1 for i in reversed(range(half))]

    def table(self):
        lines = []
        for d in range(self.dp):
            place = self.order.index(d)
            behind = [self.order[(place - r) % self.dp] for r in range(self.dp)]
            ahead = [self.order[(place + r) % self.dp] for r in range(self.dp)]
            for s in range(self.seq):
                peers = [self.peer(s, k) for k in range(self.seq)]
                lines.append([s % self.pair] + peers + behind + ahead)
        return lines

    def permute(self, array, dp_to, seq_to):
        pairs = []
        for d in range(self.dp):
            for s in range(self.seq):
                pairs.append((d * self.seq + s, dp_to(d) * self.seq + seq_to(s)))
        return lax.ppermute(array, ("dp", "seq"), pairs)

    def ring(self, array, step):
        place = {d: i for i, d in enumerate(self.order)}
        return self.permute(array, lambda d: self.order[(place[d] + step) % self.dp], lambda s: s)

    def peer(self, s, k):
        chip, core = s // self.pair, s % self.pair
        return (chip + k // self.pair) % self.chips * self.pair + (core + k % self.pair) % self.pair

    def source(self, s, k):
        chip, core = s // self.pair, s % self.pair
        return (chip - k // self.pair) % self.chips * self.pair + (core - k % self.pair) % self.pair

    def out(self, array, k):
        return self.permute(array, lambda d: d, lambda s: self.peer(s, k))

    def back(self, array, k):
        return self.permute(array, lambda d: d, lambda s: self.source(s, k))

    def swap(self, array):
        return self.out(array, 1) if self.pair == 2 else array


def gather_ring(links, piece, forward):
    found = {0: piece}
    ahead, behind = piece, piece
    for step in range(1, max(forward, links.dp - 1 - forward) + 1):
        if step <= forward:
            ahead = links.ring(ahead, 1)
            found[step] = ahead
        if step <= links.dp - 1 - forward:
            behind = links.ring(behind, -1)
            found[links.dp - step] = behind
    return [found[r] for r in range(links.dp)]


def plus(a, b):
    return (a.astype(F32) + b.astype(F32)).astype(BF)


def reduce_ring(links, blocks, forward):
    backward = links.dp - 1 - forward
    ahead = behind = None
    for step in range(max(forward, backward)):
        if step < forward:
            block = blocks[forward - step]
            ahead = block if ahead is None else plus(ahead, block)
            ahead = links.ring(ahead, 1)
        if step < backward:
            block = blocks[links.dp - (backward - step)]
            behind = block if behind is None else plus(behind, block)
            behind = links.ring(behind, -1)
    total = blocks[0].astype(F32)
    for part in (ahead, behind):
        if part is not None:
            total = total + part.astype(F32)
    return total


VMEM_SPEC = pl.BlockSpec(memory_space=pltpu.VMEM)
SMEM_SPEC = pl.BlockSpec(memory_space=pltpu.SMEM)
ANY_SPEC = pl.BlockSpec(memory_space=pl.ANY)


def at(start, size):
    return pl.ds(pl.multiple_of(start, HD), size)


def call(body, operands, specs, shapes, scratch=(), flops=0):
    moved = sum(a.size * a.dtype.itemsize for a in operands)
    moved += sum(math.prod(a.shape) * a.dtype.itemsize for a in shapes)
    return pl.pallas_call(
        body,
        in_specs=specs,
        out_specs=[VMEM_SPEC] * len(shapes),
        out_shape=shapes,
        scratch_shapes=list(scratch),
        cost_estimate=pl.CostEstimate(flops=flops + moved, bytes_accessed=moved, transcendentals=0),
        compiler_params=pltpu.CompilerParams(vmem_limit_bytes=58 * 1024 * 1024),
    )(*operands)


def cut_weights(core, lift, out, gate, pair):
    rows, units = lift.shape
    gate_rows, feat = gate.shape
    strips, part = rows // gate_rows, units // pair
    strip = feat // pair // strips
    z_part = out.shape[1] // pair

    def body(core_ref, lift_ref, out_ref, gate_ref, *outs):
        for j in range(pair):
            c = (core_ref[0] + j) % pair
            first, second = outs[2 * j], outs[2 * j + 1]
            first[:, :part] = lift_ref[:, at(c * part, part)]
            for q in range(strips):
                first[q * gate_rows : (q + 1) * gate_rows, part:] = gate_ref[
                    :, at((c * strips + q) * strip, strip)
                ]
            second[...] = out_ref[:, at(c * z_part, z_part)]

    shapes = [
        jax.ShapeDtypeStruct((rows, part + strip), BF),
        jax.ShapeDtypeStruct((out.shape[0], z_part), BF),
    ] * pair
    return call(body, (core, lift, out, gate), [SMEM_SPEC] + [VMEM_SPEC] * 3, shapes)


def pack_inputs(owners, queries, keys, values, encoder, target, width):
    tokens, z_width = encoder.shape
    n_seq = queries.shape[1] // width

    def body(owner_ref, q_ref, k_ref, v_ref, e_ref, t_ref, *outs):
        for k in range(n_seq):
            for i, ref in enumerate((q_ref, k_ref, v_ref)):
                outs[k][i] = ref[:, at(owner_ref[k] * width, width)]
        rows = outs[n_seq]
        rows[:, :z_width] = e_ref[...]
        line = lax.broadcasted_iota(jnp.int32, (tokens, tokens), 0)
        lane = lax.broadcasted_iota(jnp.int32, (tokens, tokens), 1)
        place = jnp.sum(
            jnp.where(line == lane, jnp.broadcast_to(t_ref[...], (tokens, tokens)), 0).astype(F32),
            axis=1,
            keepdims=True,
        )
        high = jnp.floor(place * (1.0 / 256.0))
        low = place - 256.0 * high
        side = lax.broadcasted_iota(jnp.int32, (tokens, HD), 1)
        rows[:, z_width:] = jnp.where(side == 0, high, jnp.where(side == 1, low, 0.0)).astype(BF)

    shapes = [jax.ShapeDtypeStruct((3, tokens, width), BF)] * n_seq
    shapes.append(jax.ShapeDtypeStruct((tokens, z_width + HD), BF))
    return call(
        body,
        (owners, queries, keys, values, encoder, target),
        [SMEM_SPEC] + [VMEM_SPEC] * 5,
        shapes,
    )


def align_features(first_token, rows, tokens, gain, bias):
    z_width = gain.shape[1]

    def body(token_ref, gain_ref, bias_ref, *refs):
        out = refs[-1]
        picked = None
        for ref in refs[:-1]:
            count = ref.shape[0]
            place = ref[:, z_width:].astype(F32)
            target = place[:, 0:1] * 256.0 + place[:, 1:2]
            here = lax.broadcasted_iota(jnp.int32, (count, tokens), 1) + token_ref[1] * tokens
            chosen = jnp.where(target == here.astype(F32), 1.0, 0.0).astype(BF)
            part = tn(chosen, ref[:, :z_width])
            picked = part if picked is None else picked + part
        centred = picked - jnp.mean(picked, axis=-1, keepdims=True)
        variance = jnp.mean(centred * centred, axis=-1, keepdims=True)
        out[...] = (
            centred * lax.rsqrt(variance + EPSILON) * gain_ref[...] + bias_ref[...]
        ).astype(BF)

    return call(
        body,
        (first_token, gain, bias, *rows),
        [SMEM_SPEC] + [VMEM_SPEC] * (2 + len(rows)),
        [jax.ShapeDtypeStruct((tokens, z_width), BF)],
        flops=2 * tokens * sum(r.shape[0] for r in rows) * z_width,
    )[0]


def project(index, spread, residual, aligned, mixed, firsts, seconds, sizes):
    n_dp, n_seq, pair, units, strips = sizes
    tokens, feat = residual.shape
    z_width = aligned.shape[1]
    width = feat // n_seq
    rows, first_cols = firsts[0][0].shape
    part, strip = units // pair, first_cols - units // pair
    out_rows, z_part = seconds[0][0].shape
    n_pieces = n_dp * pair

    def body(index_ref, spread_ref, residual_ref, aligned_ref, *refs):
        refs = list(refs)
        take = lambda n: [refs.pop(0) for _ in range(n)]
        mixed_refs, first_refs, second_refs = take(n_seq), take(n_pieces), take(n_pieces)
        sent, kept, grad_gating = take(3)
        grad_pieces = take(n_seq)
        lift, out, gate, gating, hidden, grad_hidden, sems = refs
        core = index_ref[0]

        copies = []
        for r in range(n_dp):
            d = index_ref[1 + n_seq + r]
            for j in range(pair):
                c = (core + j) % pair
                i = r * pair + j
                copies.append(
                    (
                        pltpu.make_async_copy(
                            first_refs[i].at[:, pl.ds(part, strip)],
                            gate.at[c, pl.ds(pl.multiple_of(d * rows, rows), rows), :],
                            sems.at[0, i],
                        ),
                        pltpu.make_async_copy(
                            first_refs[i].at[:, pl.ds(0, part)],
                            lift.at[pl.ds(pl.multiple_of(d * rows, rows), rows), at(c * part, part)],
                            sems.at[1, i],
                        ),
                        pltpu.make_async_copy(
                            second_refs[i],
                            out.at[
                                pl.ds(pl.multiple_of(d * out_rows, out_rows), out_rows),
                                at(c * z_part, z_part),
                            ],
                            sems.at[2, i],
                        ),
                    )
                )
        for kind in range(3):
            for copy in copies:
                copy[kind].start()
        for copy in copies:
            copy[0].wait()
        for c in range(pair):
            lines = nn(spread_ref[...], gate[c])
            for q in range(strips):
                start = (c * strips + q) * strip
                gating[:, start : start + strip] = lines[q : q + 1, :]
        for k in range(n_seq):
            here = at(index_ref[1 + k] * width, width)
            hidden[:, here] = (
                residual_ref[:, here].astype(F32) + gating[:, here] * mixed_refs[k][...].astype(F32)
            ).astype(BF)
        for copy in copies:
            copy[1].wait()
        lifted = nn(hidden[...], lift[...])
        sigmoid = 1.0 / (1.0 + jnp.exp(-lifted))
        activated = (lifted * sigmoid).astype(BF)
        slope = sigmoid * (1.0 + lifted * (1.0 - sigmoid))
        for copy in copies:
            copy[2].wait()
        predicted = nn(activated, out[...])
        target = aligned_ref[...].astype(F32)
        pred_norm = jnp.sqrt(jnp.sum(predicted * predicted, axis=1, keepdims=True) + EPSILON)
        target_norm = jnp.sqrt(jnp.sum(target * target, axis=1, keepdims=True) + EPSILON)
        cosine = jnp.sum(predicted * target, axis=1, keepdims=True) / (pred_norm * target_norm)
        scale = -1.0 * z_width / (pred_norm * target_norm)
        pull = z_width * cosine / (pred_norm * pred_norm)
        grad_pred = (scale * target + pull * predicted).astype(BF)
        grad_lifted = (nt(grad_pred, out[...]) * slope).astype(BF)
        sent[:, :feat] = hidden[...]
        sent[:, feat : feat + units] = activated
        grad_hidden[...] = nt(grad_lifted, lift[...])
        lift[:tokens, :units] = grad_lifted
        out[:tokens, :z_width] = grad_pred
        other = (core + pair - 1) % pair
        sent[:, feat + units : feat + units + part] = lift[:tokens, at(other * part, part)]
        sent[:, feat + units + part :] = out[:tokens, at(other * z_part, z_part)]
        kept[:, :part] = lift[:tokens, at(core * part, part)]
        kept[:, part:] = out[:tokens, at(core * z_part, z_part)]
        for k in range(n_seq):
            here = at(index_ref[1 + k] * width, width)
            grads = grad_hidden[:, here]
            grad_pieces[k][...] = (gating[:, here] * grads).astype(BF)
            grad_gating[:, here] = jnp.sum(
                grads * mixed_refs[k][...].astype(F32), axis=0, keepdims=True
            )

    shapes = [
        jax.ShapeDtypeStruct((tokens, feat + units + part + z_part), BF),
        jax.ShapeDtypeStruct((tokens, part + z_part), BF),
        jax.ShapeDtypeStruct((1, feat), F32),
    ] + [jax.ShapeDtypeStruct((tokens, width), BF)] * n_seq
    flat = lambda pieces: [p for both in pieces for p in both]
    return call(
        body,
        (index, spread, residual, aligned, *mixed, *flat(firsts), *flat(seconds)),
        [SMEM_SPEC] + [VMEM_SPEC] * (3 + n_seq) + [ANY_SPEC] * (2 * n_pieces),
        shapes,
        [
            pltpu.VMEM((n_dp * rows, units), BF),
            pltpu.VMEM((n_dp * out_rows, z_width), BF),
            pltpu.VMEM((pair, n_dp * rows, strip), BF),
            pltpu.VMEM((1, feat), F32),
            pltpu.VMEM((tokens, feat), BF),
            pltpu.VMEM((tokens, feat), F32),
            pltpu.SemaphoreType.DMA((3, n_pieces)),
        ],
        flops=6 * tokens * units * (feat + z_width),
    )


def out_blocks(index, sent, got, kept, sizes, z_part, out_rows):
    n_dp, n_seq, pair, units, _ = sizes
    tokens, cols = sent.shape
    act = cols - units - units // pair - z_part
    halves = [sent] if got is None else [sent, got]

    def body(index_ref, kept_ref, *refs):
        sources, outs = refs[: len(halves)], refs[len(halves) :]
        grads = [kept_ref[:, units // pair :]]
        if got is not None:
            grads.append(sources[1][:, cols - z_part :])
        grads = jnp.concatenate(grads, axis=0)
        for r in range(n_dp):
            here = at(act + index_ref[1 + n_seq + n_dp + r] * out_rows, out_rows)
            left = jnp.concatenate([s[:, here] for s in sources], axis=0)
            outs[r][...] = tn(left, grads).astype(BF)

    return call(
        body,
        (index, kept, *halves),
        [SMEM_SPEC] + [VMEM_SPEC] * (1 + len(halves)),
        [jax.ShapeDtypeStruct((out_rows, z_part), BF)] * n_dp,
        flops=4 * tokens * z_part * units,
    )


def lift_blocks(index, sent, got, kept, grad_gating, embedded, sizes, rows, strip):
    n_dp, n_seq, pair, units, strips = sizes
    tokens, feat = sent.shape[0], n_dp * rows
    part, gate_rows = units // pair, rows // strips
    halves = [sent] if got is None else [sent, got]
    sums = len(grad_gating)

    def body(index_ref, kept_ref, embedded_ref, *refs):
        gating_refs, sources, outs = refs[:sums], refs[sums : sums + len(halves)], refs[sums + len(halves) :]
        grads = [kept_ref[:, :part]]
        if got is not None:
            grads.append(sources[1][:, feat + units : feat + units + part])
        grads = jnp.concatenate(grads, axis=0)
        core = index_ref[0]
        for r in range(n_dp):
            d = index_ref[1 + n_seq + n_dp + r]
            here = at(d * rows, rows)
            left = jnp.concatenate([s[:, here] for s in sources], axis=0)
            outs[r][:, :part] = tn(left, grads).astype(BF)
            line = embedded_ref[pl.ds(pl.multiple_of(d * gate_rows, gate_rows), gate_rows), :]
            for q in range(strips):
                there = at((core * strips + q) * strip, strip)
                gate = sum(g[:, there] for g in gating_refs)
                outs[r][q * gate_rows : (q + 1) * gate_rows, part:] = (line * gate).astype(BF)

    return call(
        body,
        (index, kept, embedded, *grad_gating, *halves),
        [SMEM_SPEC] + [VMEM_SPEC] * (2 + sums + len(halves)),
        [jax.ShapeDtypeStruct((rows, part + strip), BF)] * n_dp,
        flops=4 * tokens * part * feat,
    )


def place_lift(core, shares, sizes):
    _, _, pair, units, strips = sizes
    rows, cols = shares[0].shape
    part, strip = units // pair, cols - units // pair
    gate_rows = rows // strips

    def body(core_ref, *refs):
        shares_refs, (gate, lift) = refs[:pair], refs[pair:]
        for j in range(pair):
            c = (core_ref[0] + j) % pair
            lift[:, at(c * part, part)] = shares_refs[j][:, :part].astype(F32)
            for q in range(strips):
                gate[:, at((c * strips + q) * strip, strip)] = shares_refs[j][
                    q * gate_rows : (q + 1) * gate_rows, part:
                ].astype(F32)

    return call(
        body,
        (core, *shares),
        [SMEM_SPEC] + [VMEM_SPEC] * pair,
        [
            jax.ShapeDtypeStruct((gate_rows, strip * strips * pair), F32),
            jax.ShapeDtypeStruct((rows, units), F32),
        ],
    )


def place_out(core, shares, pair):
    out_rows, z_part = shares[0].shape

    def body(core_ref, *refs):
        for j in range(pair):
            c = (core_ref[0] + j) % pair
            refs[pair][:, at(c * z_part, z_part)] = refs[j][...].astype(F32)

    return call(
        body,
        (core, *shares),
        [SMEM_SPEC] + [VMEM_SPEC] * pair,
        [jax.ShapeDtypeStruct((out_rows, z_part * pair), F32)],
    )[0]


def place_grads(owners, pieces):
    _, tokens, width = pieces[0].shape

    def body(owner_ref, *refs):
        sources, outs = refs[: len(pieces)], refs[len(pieces) :]
        for k, ref in enumerate(sources):
            for i in range(3):
                outs[i][:, at(owner_ref[k] * width, width)] = ref[i]

    return call(
        body,
        (owners, *pieces),
        [SMEM_SPEC] + [VMEM_SPEC] * len(pieces),
        [jax.ShapeDtypeStruct((tokens, width * len(pieces)), BF)] * 3,
    )


def step(
    queries,
    key_states,
    value_states,
    residual,
    enc_hidden,
    enc_gain,
    enc_bias,
    feature_target,
    timestep,
    gate_weight,
    lift_weight,
    out_weight,
):
    links = Links()
    n_dp, n_seq, pair = links.dp, links.seq, links.pair
    tokens, feat = queries.shape[1:]
    width = feat // n_seq
    rows, units = lift_weight.shape
    gate_rows = gate_weight.shape[0]
    temb, strips = gate_rows * n_dp, rows // gate_rows
    sizes = (n_dp, n_seq, pair, units, strips)
    order = sorted(range(1, n_seq), key=lambda k: (k < pair, k))
    index = lax.dynamic_index_in_dim(
        jnp.asarray(links.table(), jnp.int32), links.d * n_seq + links.s, 0, False
    )
    owner_index = index[1 : 1 + n_seq]

    halves = cut_weights(index, lift_weight, out_weight, gate_weight, pair)
    ahead = n_dp // 2
    first_parts = gather_ring(links, halves[0], ahead)
    second_parts = gather_ring(links, halves[1], n_dp - 1 - ahead)

    def with_other(parts, own):
        if pair == 1:
            return [[p] for p in parts]
        return [[parts[0], own]] + [[p, links.swap(p)] for p in parts[1:]]

    firsts = with_other(first_parts, halves[2 * pair - 2])
    seconds = with_other(second_parts, halves[2 * pair - 1])

    packed = pack_inputs(
        owner_index,
        queries[0],
        key_states[0],
        value_states[0],
        enc_hidden[0],
        feature_target,
        width,
    )
    packs = [packed[0]] + [None] * (n_seq - 1)
    for k in order:
        packs[k] = links.out(packed[k], k)
    clip_rows = [packed[n_seq]]
    clip_rows += [links.out(packed[n_seq], j * pair) for j in range(1, links.chips)]
    if pair == 2:
        clip_rows += [links.swap(r) for r in clip_rows]
    aligned = align_features(
        index,
        clip_rows,
        tokens,
        enc_gain[None],
        enc_bias[None],
    )

    embedded = embed_time(timestep, temb)
    spread = (
        embedded.reshape(n_dp, 1, 1, gate_rows) * jnp.eye(strips, dtype=BF)[None, :, :, None]
    )
    spread = spread.transpose(1, 0, 2, 3).reshape(strips, n_dp * rows)
    tall = jnp.broadcast_to(embedded.astype(F32).reshape(temb, 1), (temb, feat // pair // strips))

    attended = attention_forward(packs)
    mixed = [attended[0]] + [None] * (n_seq - 1)
    for k in order:
        mixed[k] = links.back(attended[k], k)

    sent, kept, grad_gating, *pieces = project(
        index, spread, residual[0], aligned, mixed, firsts, seconds, sizes
    )
    got, gatings = None, [grad_gating]
    if pair == 2:
        got = links.swap(sent)
        gatings.append(links.swap(grad_gating))
    grads = [pieces[0]] + [None] * (n_seq - 1)
    for k in order:
        grads[k] = links.out(pieces[k], k)

    part_out = out_blocks(
        index, sent, got, kept, sizes, halves[1].shape[1], halves[1].shape[0]
    )
    part_lift = lift_blocks(
        index, sent, got, kept, gatings, tall, sizes, rows, feat // pair // strips
    )
    share_second = reduce_ring(links, part_out, n_dp - 1 - ahead)
    share_first = reduce_ring(links, part_lift, ahead)

    def over_seq(share):
        mine = share.astype(BF)
        total = share
        for j in range(1, links.chips):
            total = total + links.out(mine, j * pair).astype(F32)
        mine = total.astype(BF)
        return [mine] if pair == 1 else [mine, links.swap(mine)]

    grad_gate, grad_lift = place_lift(index, over_seq(share_first), sizes)
    grad_out = place_out(index, over_seq(share_second), pair)

    back = attention_backward(packs, grads, part_lift[0])
    done = [back[0]] + [None] * (n_seq - 1)
    for k in order:
        done[k] = links.back(back[k], k)
    d_queries, d_keys, d_values = place_grads(owner_index, done)
    return (d_queries[None], d_keys[None], d_values[None], grad_gate, grad_lift, grad_out)


def solution(mesh):
    in_specs = (
        P("dp", "seq", None),
        P("dp", "seq", None),
        P("dp", "seq", None),
        P("dp", "seq", None),
        P("dp", "seq", None),
        P(),
        P(),
        P("dp", "seq"),
        P("dp"),
        P("dp", None),
        P("dp", None),
        P("dp", None),
    )
    out_specs = (
        P("dp", "seq", None),
        P("dp", "seq", None),
        P("dp", "seq", None),
        P("dp", None),
        P("dp", None),
        P("dp", None),
    )
    return jax.shard_map(step, mesh=mesh, in_specs=in_specs, out_specs=out_specs, check_vma=False)
```

```python
import functools
import math

import jax
import jax.numpy as jnp
from jax import lax
from jax.experimental import pallas as pl
from jax.experimental.pallas import tpu as pltpu
from jax.sharding import PartitionSpec as P


HD = 128
EPSILON = 1e-06
BF = jnp.bfloat16
F32 = jnp.float32


def embed_time(timestep, width):
    half_width = width // 2
    frequency = jnp.exp(
        -math.log(10000.0) * jnp.arange(half_width).astype(F32) / half_width
    )
    angles = timestep.astype(F32)[:, None] * frequency[None, :]
    return jnp.concatenate([jnp.cos(angles), jnp.sin(angles)], axis=1).astype(BF)


def nt(a, b):
    return lax.dot_general(a, b, (((1,), (1,)), ((), ())), preferred_element_type=F32)


def nn(a, b):
    return lax.dot_general(a, b, (((1,), (0,)), ((), ())), preferred_element_type=F32)


def tn(a, b):
    return lax.dot_general(a, b, (((0,), (0,)), ((), ())), preferred_element_type=F32)


def group_of(tokens, blocks):
    count = max(1, 256 // tokens)
    return count if blocks % count == 0 else 1


def joined(parts):
    return parts[0] if len(parts) == 1 else jnp.concatenate(parts, axis=0)


SCALE = HD ** (-0.5)


def soft_columns(keys, query):
    scores = nt(keys, query)
    shifted = jnp.exp2(
        (scores - jnp.max(scores, axis=0, keepdims=True)) * (SCALE * math.log2(math.e))
    )
    return shifted, 1.0 / jnp.sum(shifted, axis=0, keepdims=True)


def forward_body(blocks, *refs):
    packs, outs = refs[:blocks], refs[blocks:]
    tokens = packs[0].shape[1]
    step = group_of(tokens, blocks)
    keys = joined([p[1] for p in packs])
    values = joined([p[2] for p in packs])
    for first in range(0, blocks, step):
        shifted, inverse = soft_columns(keys, joined([p[0] for p in packs[first : first + step]]))
        mixed = (tn(values, shifted.astype(BF)) * inverse).T.astype(BF)
        for i in range(step):
            outs[first + i][...] = mixed[i * tokens : (i + 1) * tokens]


def attention_forward(packs):
    blocks = len(packs)
    _, tokens, width = packs[0].shape
    heads = width // HD
    return pl.pallas_call(
        functools.partial(forward_body, blocks),
        grid=(heads,),
        in_specs=[pl.BlockSpec((3, tokens, HD), lambda h: (0, 0, h))] * blocks,
        out_specs=[pl.BlockSpec((tokens, HD), lambda h: (0, h))] * blocks,
        out_shape=[jax.ShapeDtypeStruct((tokens, width), BF)] * blocks,
        cost_estimate=pl.CostEstimate(
            flops=4 * heads * (blocks * tokens) ** 2 * HD,
            bytes_accessed=8 * blocks * tokens * width,
            transcendentals=heads * (blocks * tokens) ** 2,
        ),
        name="attend",
    )(*packs)


def backward_body(blocks, *refs):
    packs, grads, outs = refs[:blocks], refs[blocks : 2 * blocks], refs[2 * blocks + 1 :]
    tokens = packs[0].shape[1]
    step = group_of(tokens, blocks)
    keys = joined([p[1] for p in packs])
    values = joined([p[2] for p in packs])
    grad_keys = grad_values = None
    for first in range(0, blocks, step):
        query = joined([p[0] for p in packs[first : first + step]])
        grad_rows = joined([g[...] for g in grads[first : first + step]])
        shifted, inverse = soft_columns(keys, query)
        chances = shifted * inverse
        grad_chances = nt(values, grad_rows)
        add_values = nn(chances.astype(BF), grad_rows)
        inner = jnp.sum(grad_chances * chances, axis=0, keepdims=True)
        grad_scores = (chances * (grad_chances - inner)).astype(BF)
        grad_query = (tn(keys, grad_scores) * SCALE).T.astype(BF)
        for i in range(step):
            outs[first + i][0] = grad_query[i * tokens : (i + 1) * tokens]
        add_keys = nn(grad_scores, query)
        grad_keys = add_keys if grad_keys is None else grad_keys + add_keys
        grad_values = add_values if grad_values is None else grad_values + add_values
    for place, out in enumerate(outs):
        out[1] = (grad_keys[place * tokens : (place + 1) * tokens] * SCALE).astype(BF)
        out[2] = grad_values[place * tokens : (place + 1) * tokens].astype(BF)


def attention_backward(packs, grads, after):
    blocks = len(packs)
    _, tokens, width = packs[0].shape
    heads = width // HD
    pack_spec = pl.BlockSpec((3, tokens, HD), lambda h: (0, 0, h))
    row_spec = pl.BlockSpec((tokens, HD), lambda h: (0, h))
    return pl.pallas_call(
        functools.partial(backward_body, blocks),
        grid=(heads,),
        in_specs=[pack_spec] * blocks + [row_spec] * blocks + [pl.BlockSpec(memory_space=pl.ANY)],
        out_specs=[pack_spec] * blocks,
        out_shape=[jax.ShapeDtypeStruct((3, tokens, width), BF)] * blocks,
        cost_estimate=pl.CostEstimate(
            flops=10 * heads * (blocks * tokens) ** 2 * HD,
            bytes_accessed=14 * blocks * tokens * width,
            transcendentals=heads * (blocks * tokens) ** 2,
        ),
        name="attend_back",
    )(*packs, *grads, after)


class Links:
    def __init__(self):
        self.dp, self.seq = lax.axis_size("dp"), lax.axis_size("seq")
        self.pair = 2 if self.seq % 2 == 0 else 1
        self.chips = self.seq // self.pair
        self.d, self.s = lax.axis_index("dp"), lax.axis_index("seq")
        half = self.dp // 2
        if self.dp % 2:
            self.order = list(range(self.dp))
        else:
            self.order = [2 * i for i in range(half)] + [2 * i + 1 for i in reversed(range(half))]

    def table(self):
        lines = []
        for d in range(self.dp):
            place = self.order.index(d)
            behind = [self.order[(place - r) % self.dp] for r in range(self.dp)]
            ahead = [self.order[(place + r) % self.dp] for r in range(self.dp)]
            for s in range(self.seq):
                peers = [self.peer(s, k) for k in range(self.seq)]
                lines.append([s % self.pair] + peers + behind + ahead)
        return lines

    def permute(self, array, dp_to, seq_to):
        pairs = []
        for d in range(self.dp):
            for s in range(self.seq):
                pairs.append((d * self.seq + s, dp_to(d) * self.seq + seq_to(s)))
        return lax.ppermute(array, ("dp", "seq"), pairs)

    def ring(self, array, step):
        place = {d: i for i, d in enumerate(self.order)}
        return self.permute(array, lambda d: self.order[(place[d] + step) % self.dp], lambda s: s)

    def peer(self, s, k):
        chip, core = s // self.pair, s % self.pair
        return (chip + k // self.pair) % self.chips * self.pair + (core + k % self.pair) % self.pair

    def source(self, s, k):
        chip, core = s // self.pair, s % self.pair
        return (chip - k // self.pair) % self.chips * self.pair + (core - k % self.pair) % self.pair

    def out(self, array, k):
        return self.permute(array, lambda d: d, lambda s: self.peer(s, k))

    def back(self, array, k):
        return self.permute(array, lambda d: d, lambda s: self.source(s, k))

    def swap(self, array):
        return self.out(array, 1) if self.pair == 2 else array


def gather_ring(links, piece, forward):
    found = {0: piece}
    ahead, behind = piece, piece
    for step in range(1, max(forward, links.dp - 1 - forward) + 1):
        if step <= forward:
            ahead = links.ring(ahead, 1)
            found[step] = ahead
        if step <= links.dp - 1 - forward:
            behind = links.ring(behind, -1)
            found[links.dp - step] = behind
    return [found[r] for r in range(links.dp)]


def plus(a, b):
    return (a.astype(F32) + b.astype(F32)).astype(BF)


def reduce_ring(links, blocks, forward):
    backward = links.dp - 1 - forward
    ahead = behind = None
    for step in range(max(forward, backward)):
        if step < forward:
            block = blocks[forward - step]
            ahead = block if ahead is None else plus(ahead, block)
            ahead = links.ring(ahead, 1)
        if step < backward:
            block = blocks[links.dp - (backward - step)]
            behind = block if behind is None else plus(behind, block)
            behind = links.ring(behind, -1)
    total = blocks[0].astype(F32)
    for part in (ahead, behind):
        if part is not None:
            total = total + part.astype(F32)
    return total


VMEM_SPEC = pl.BlockSpec(memory_space=pltpu.VMEM)
SMEM_SPEC = pl.BlockSpec(memory_space=pltpu.SMEM)
ANY_SPEC = pl.BlockSpec(memory_space=pl.ANY)


def at(start, size):
    return pl.ds(pl.multiple_of(start, HD), size)


def call(body, operands, specs, shapes, scratch=(), flops=0):
    moved = sum(a.size * a.dtype.itemsize for a in operands)
    moved += sum(math.prod(a.shape) * a.dtype.itemsize for a in shapes)
    return pl.pallas_call(
        body,
        in_specs=specs,
        out_specs=[VMEM_SPEC] * len(shapes),
        out_shape=shapes,
        scratch_shapes=list(scratch),
        cost_estimate=pl.CostEstimate(flops=flops + moved, bytes_accessed=moved, transcendentals=0),
        compiler_params=pltpu.CompilerParams(vmem_limit_bytes=58 * 1024 * 1024),
    )(*operands)


def cut_weights(core, lift, out, gate, pair):
    rows, units = lift.shape
    gate_rows, feat = gate.shape
    strips, part = rows // gate_rows, units // pair
    strip = feat // pair // strips
    z_part = out.shape[1] // pair

    def body(core_ref, lift_ref, out_ref, gate_ref, *outs):
        for j in range(pair):
            c = (core_ref[0] + j) % pair
            first, second = outs[2 * j], outs[2 * j + 1]
            first[:, :part] = lift_ref[:, at(c * part, part)]
            for q in range(strips):
                first[q * gate_rows : (q + 1) * gate_rows, part:] = gate_ref[
                    :, at((c * strips + q) * strip, strip)
                ]
            second[...] = out_ref[:, at(c * z_part, z_part)]

    shapes = [
        jax.ShapeDtypeStruct((rows, part + strip), BF),
        jax.ShapeDtypeStruct((out.shape[0], z_part), BF),
    ] * pair
    return call(body, (core, lift, out, gate), [SMEM_SPEC] + [VMEM_SPEC] * 3, shapes)


def pack_inputs(owners, queries, keys, values, encoder, target, width):
    tokens, z_width = encoder.shape
    n_seq = queries.shape[1] // width

    def body(owner_ref, q_ref, k_ref, v_ref, e_ref, t_ref, *outs):
        for k in range(n_seq):
            for i, ref in enumerate((q_ref, k_ref, v_ref)):
                outs[k][i] = ref[:, at(owner_ref[k] * width, width)]
        rows = outs[n_seq]
        rows[:, :z_width] = e_ref[...]
        line = lax.broadcasted_iota(jnp.int32, (tokens, tokens), 0)
        lane = lax.broadcasted_iota(jnp.int32, (tokens, tokens), 1)
        place = jnp.sum(
            jnp.where(line == lane, jnp.broadcast_to(t_ref[...], (tokens, tokens)), 0).astype(F32),
            axis=1,
            keepdims=True,
        )
        high = jnp.floor(place * (1.0 / 256.0))
        low = place - 256.0 * high
        side = lax.broadcasted_iota(jnp.int32, (tokens, HD), 1)
        rows[:, z_width:] = jnp.where(side == 0, high, jnp.where(side == 1, low, 0.0)).astype(BF)

    shapes = [jax.ShapeDtypeStruct((3, tokens, width), BF)] * n_seq
    shapes.append(jax.ShapeDtypeStruct((tokens, z_width + HD), BF))
    return call(
        body,
        (owners, queries, keys, values, encoder, target),
        [SMEM_SPEC] + [VMEM_SPEC] * 5,
        shapes,
    )


def align_features(first_token, rows, tokens, gain, bias):
    z_width = gain.shape[1]

    def body(token_ref, gain_ref, bias_ref, *refs):
        out = refs[-1]
        picked = None
        for ref in refs[:-1]:
            count = ref.shape[0]
            place = ref[:, z_width:].astype(F32)
            target = place[:, 0:1] * 256.0 + place[:, 1:2]
            here = lax.broadcasted_iota(jnp.int32, (count, tokens), 1) + token_ref[1] * tokens
            chosen = jnp.where(target == here.astype(F32), 1.0, 0.0).astype(BF)
            part = tn(chosen, ref[:, :z_width])
            picked = part if picked is None else picked + part
        centred = picked - jnp.mean(picked, axis=-1, keepdims=True)
        variance = jnp.mean(centred * centred, axis=-1, keepdims=True)
        out[...] = (
            centred * lax.rsqrt(variance + EPSILON) * gain_ref[...] + bias_ref[...]
        ).astype(BF)

    return call(
        body,
        (first_token, gain, bias, *rows),
        [SMEM_SPEC] + [VMEM_SPEC] * (2 + len(rows)),
        [jax.ShapeDtypeStruct((tokens, z_width), BF)],
        flops=2 * tokens * sum(r.shape[0] for r in rows) * z_width,
    )[0]


def project(index, spread, residual, aligned, mixed, firsts, seconds, sizes):
    n_dp, n_seq, pair, units, strips = sizes
    tokens, feat = residual.shape
    z_width = aligned.shape[1]
    width = feat // n_seq
    rows, first_cols = firsts[0][0].shape
    part, strip = units // pair, first_cols - units // pair
    out_rows, z_part = seconds[0][0].shape
    n_pieces = n_dp * pair

    def body(index_ref, spread_ref, residual_ref, aligned_ref, *refs):
        refs = list(refs)
        take = lambda n: [refs.pop(0) for _ in range(n)]
        mixed_refs, first_refs, second_refs = take(n_seq), take(n_pieces), take(n_pieces)
        sent, kept, grad_gating = take(3)
        grad_pieces = take(n_seq)
        lift, out, gate, gating, hidden, grad_hidden, sems = refs
        core = index_ref[0]

        copies = []
        for r in range(n_dp):
            d = index_ref[1 + n_seq + r]
            for j in range(pair):
                c = (core + j) % pair
                i = r * pair + j
                copies.append(
                    (
                        pltpu.make_async_copy(
                            first_refs[i].at[:, pl.ds(part, strip)],
                            gate.at[c, pl.ds(pl.multiple_of(d * rows, rows), rows), :],
                            sems.at[0, i],
                        ),
                        pltpu.make_async_copy(
                            first_refs[i].at[:, pl.ds(0, part)],
                            lift.at[pl.ds(pl.multiple_of(d * rows, rows), rows), at(c * part, part)],
                            sems.at[1, i],
                        ),
                        pltpu.make_async_copy(
                            second_refs[i],
                            out.at[
                                pl.ds(pl.multiple_of(d * out_rows, out_rows), out_rows),
                                at(c * z_part, z_part),
                            ],
                            sems.at[2, i],
                        ),
                    )
                )
        for kind in range(3):
            for copy in copies:
                copy[kind].start()
        for copy in copies:
            copy[0].wait()
        for c in range(pair):
            lines = nn(spread_ref[...], gate[c])
            for q in range(strips):
                start = (c * strips + q) * strip
                gating[:, start : start + strip] = lines[q : q + 1, :]
        for k in range(n_seq):
            here = at(index_ref[1 + k] * width, width)
            hidden[:, here] = (
                residual_ref[:, here].astype(F32) + gating[:, here] * mixed_refs[k][...].astype(F32)
            ).astype(BF)
        for copy in copies:
            copy[1].wait()
        lifted = nn(hidden[...], lift[...])
        sigmoid = 1.0 / (1.0 + jnp.exp(-lifted))
        activated = (lifted * sigmoid).astype(BF)
        slope = sigmoid * (1.0 + lifted * (1.0 - sigmoid))
        for copy in copies:
            copy[2].wait()
        predicted = nn(activated, out[...])
        target = aligned_ref[...].astype(F32)
        pred_norm = jnp.sqrt(jnp.sum(predicted * predicted, axis=1, keepdims=True) + EPSILON)
        target_norm = jnp.sqrt(jnp.sum(target * target, axis=1, keepdims=True) + EPSILON)
        cosine = jnp.sum(predicted * target, axis=1, keepdims=True) / (pred_norm * target_norm)
        scale = -1.0 * z_width / (pred_norm * target_norm)
        pull = z_width * cosine / (pred_norm * pred_norm)
        grad_pred = (scale * target + pull * predicted).astype(BF)
        grad_lifted = (nt(grad_pred, out[...]) * slope).astype(BF)
        sent[:, :feat] = hidden[...]
        sent[:, feat : feat + units] = activated
        grad_hidden[...] = nt(grad_lifted, lift[...])
        lift[:tokens, :units] = grad_lifted
        out[:tokens, :z_width] = grad_pred
        other = (core + pair - 1) % pair
        sent[:, feat + units : feat + units + part] = lift[:tokens, at(other * part, part)]
        sent[:, feat + units + part :] = out[:tokens, at(other * z_part, z_part)]
        kept[:, :part] = lift[:tokens, at(core * part, part)]
        kept[:, part:] = out[:tokens, at(core * z_part, z_part)]
        for k in range(n_seq):
            here = at(index_ref[1 + k] * width, width)
            grads = grad_hidden[:, here]
            grad_pieces[k][...] = (gating[:, here] * grads).astype(BF)
            grad_gating[:, here] = jnp.sum(
                grads * mixed_refs[k][...].astype(F32), axis=0, keepdims=True
            )

    shapes = [
        jax.ShapeDtypeStruct((tokens, feat + units + part + z_part), BF),
        jax.ShapeDtypeStruct((tokens, part + z_part), BF),
        jax.ShapeDtypeStruct((1, feat), F32),
    ] + [jax.ShapeDtypeStruct((tokens, width), BF)] * n_seq
    flat = lambda pieces: [p for both in pieces for p in both]
    return call(
        body,
        (index, spread, residual, aligned, *mixed, *flat(firsts), *flat(seconds)),
        [SMEM_SPEC] + [VMEM_SPEC] * (3 + n_seq) + [ANY_SPEC] * (2 * n_pieces),
        shapes,
        [
            pltpu.VMEM((n_dp * rows, units), BF),
            pltpu.VMEM((n_dp * out_rows, z_width), BF),
            pltpu.VMEM((pair, n_dp * rows, strip), BF),
            pltpu.VMEM((1, feat), F32),
            pltpu.VMEM((tokens, feat), BF),
            pltpu.VMEM((tokens, feat), F32),
            pltpu.SemaphoreType.DMA((3, n_pieces)),
        ],
        flops=6 * tokens * units * (feat + z_width),
    )


def out_blocks(index, sent, got, kept, sizes, z_part, out_rows):
    n_dp, n_seq, pair, units, _ = sizes
    tokens, cols = sent.shape
    act = cols - units - units // pair - z_part
    halves = [sent] if got is None else [sent, got]

    def body(index_ref, kept_ref, *refs):
        sources, outs = refs[: len(halves)], refs[len(halves) :]
        grads = [kept_ref[:, units // pair :]]
        if got is not None:
            grads.append(sources[1][:, cols - z_part :])
        grads = jnp.concatenate(grads, axis=0)
        for r in range(n_dp):
            here = at(act + index_ref[1 + n_seq + n_dp + r] * out_rows, out_rows)
            left = jnp.concatenate([s[:, here] for s in sources], axis=0)
            outs[r][...] = tn(left, grads).astype(BF)

    return call(
        body,
        (index, kept, *halves),
        [SMEM_SPEC] + [VMEM_SPEC] * (1 + len(halves)),
        [jax.ShapeDtypeStruct((out_rows, z_part), BF)] * n_dp,
        flops=4 * tokens * z_part * units,
    )


def lift_blocks(index, sent, got, kept, grad_gating, embedded, sizes, rows, strip):
    n_dp, n_seq, pair, units, strips = sizes
    tokens, feat = sent.shape[0], n_dp * rows
    part, gate_rows = units // pair, rows // strips
    halves = [sent] if got is None else [sent, got]
    sums = len(grad_gating)

    def body(index_ref, kept_ref, embedded_ref, *refs):
        gating_refs, sources, outs = refs[:sums], refs[sums : sums + len(halves)], refs[sums + len(halves) :]
        grads = [kept_ref[:, :part]]
        if got is not None:
            grads.append(sources[1][:, feat + units : feat + units + part])
        grads = jnp.concatenate(grads, axis=0)
        core = index_ref[0]
        for r in range(n_dp):
            d = index_ref[1 + n_seq + n_dp + r]
            here = at(d * rows, rows)
            left = jnp.concatenate([s[:, here] for s in sources], axis=0)
            outs[r][:, :part] = tn(left, grads).astype(BF)
            line = embedded_ref[pl.ds(pl.multiple_of(d * gate_rows, gate_rows), gate_rows), :]
            for q in range(strips):
                there = at((core * strips + q) * strip, strip)
                gate = sum(g[:, there] for g in gating_refs)
                outs[r][q * gate_rows : (q + 1) * gate_rows, part:] = (line * gate).astype(BF)

    return call(
        body,
        (index, kept, embedded, *grad_gating, *halves),
        [SMEM_SPEC] + [VMEM_SPEC] * (2 + sums + len(halves)),
        [jax.ShapeDtypeStruct((rows, part + strip), BF)] * n_dp,
        flops=4 * tokens * part * feat,
    )


def place_lift(core, shares, sizes):
    _, _, pair, units, strips = sizes
    rows, cols = shares[0].shape
    part, strip = units // pair, cols - units // pair
    gate_rows = rows // strips

    def body(core_ref, *refs):
        shares_refs, (gate, lift) = refs[:pair], refs[pair:]
        for j in range(pair):
            c = (core_ref[0] + j) % pair
            lift[:, at(c * part, part)] = shares_refs[j][:, :part].astype(F32)
            for q in range(strips):
                gate[:, at((c * strips + q) * strip, strip)] = shares_refs[j][
                    q * gate_rows : (q + 1) * gate_rows, part:
                ].astype(F32)

    return call(
        body,
        (core, *shares),
        [SMEM_SPEC] + [VMEM_SPEC] * pair,
        [
            jax.ShapeDtypeStruct((gate_rows, strip * strips * pair), F32),
            jax.ShapeDtypeStruct((rows, units), F32),
        ],
    )


def place_out(core, shares, pair):
    out_rows, z_part = shares[0].shape

    def body(core_ref, *refs):
        for j in range(pair):
            c = (core_ref[0] + j) % pair
            refs[pair][:, at(c * z_part, z_part)] = refs[j][...].astype(F32)

    return call(
        body,
        (core, *shares),
        [SMEM_SPEC] + [VMEM_SPEC] * pair,
        [jax.ShapeDtypeStruct((out_rows, z_part * pair), F32)],
    )[0]


def place_grads(owners, pieces):
    _, tokens, width = pieces[0].shape

    def body(owner_ref, *refs):
        sources, outs = refs[: len(pieces)], refs[len(pieces) :]
        for k, ref in enumerate(sources):
            for i in range(3):
                outs[i][:, at(owner_ref[k] * width, width)] = ref[i]

    return call(
        body,
        (owners, *pieces),
        [SMEM_SPEC] + [VMEM_SPEC] * len(pieces),
        [jax.ShapeDtypeStruct((tokens, width * len(pieces)), BF)] * 3,
    )


def step(
    queries,
    key_states,
    value_states,
    residual,
    enc_hidden,
    enc_gain,
    enc_bias,
    feature_target,
    timestep,
    gate_weight,
    lift_weight,
    out_weight,
):
    links = Links()
    n_dp, n_seq, pair = links.dp, links.seq, links.pair
    tokens, feat = queries.shape[1:]
    width = feat // n_seq
    rows, units = lift_weight.shape
    gate_rows = gate_weight.shape[0]
    temb, strips = gate_rows * n_dp, rows // gate_rows
    sizes = (n_dp, n_seq, pair, units, strips)
    order = sorted(range(1, n_seq), key=lambda k: (k < pair, k))
    index = lax.dynamic_index_in_dim(
        jnp.asarray(links.table(), jnp.int32), links.d * n_seq + links.s, 0, False
    )
    owner_index = index[1 : 1 + n_seq]

    halves = cut_weights(index, lift_weight, out_weight, gate_weight, pair)
    ahead = n_dp // 2
    first_parts = gather_ring(links, halves[0], ahead)
    second_parts = gather_ring(links, halves[1], n_dp - 1 - ahead)

    def with_other(parts, own):
        if pair == 1:
            return [[p] for p in parts]
        return [[parts[0], own]] + [[p, links.swap(p)] for p in parts[1:]]

    firsts = with_other(first_parts, halves[2 * pair - 2])
    seconds = with_other(second_parts, halves[2 * pair - 1])

    packed = pack_inputs(
        owner_index,
        queries[0],
        key_states[0],
        value_states[0],
        enc_hidden[0],
        feature_target,
        width,
    )
    packs = [packed[0]] + [None] * (n_seq - 1)
    for k in order:
        packs[k] = links.out(packed[k], k)
    clip_rows = [packed[n_seq]]
    clip_rows += [links.out(packed[n_seq], j * pair) for j in range(1, links.chips)]
    if pair == 2:
        clip_rows += [links.swap(r) for r in clip_rows]
    aligned = align_features(
        index,
        clip_rows,
        tokens,
        enc_gain[None],
        enc_bias[None],
    )

    embedded = embed_time(timestep, temb)
    spread = (
        embedded.reshape(n_dp, 1, 1, gate_rows) * jnp.eye(strips, dtype=BF)[None, :, :, None]
    )
    spread = spread.transpose(1, 0, 2, 3).reshape(strips, n_dp * rows)
    tall = jnp.broadcast_to(embedded.astype(F32).reshape(temb, 1), (temb, feat // pair // strips))

    attended = attention_forward(packs)
    mixed = [attended[0]] + [None] * (n_seq - 1)
    for k in order:
        mixed[k] = links.back(attended[k], k)

    sent, kept, grad_gating, *pieces = project(
        index, spread, residual[0], aligned, mixed, firsts, seconds, sizes
    )
    got, gatings = None, [grad_gating]
    if pair == 2:
        got = links.swap(sent)
        gatings.append(links.swap(grad_gating))
    grads = [pieces[0]] + [None] * (n_seq - 1)
    for k in order:
        grads[k] = links.out(pieces[k], k)

    part_out = out_blocks(
        index, sent, got, kept, sizes, halves[1].shape[1], halves[1].shape[0]
    )
    part_lift = lift_blocks(
        index, sent, got, kept, gatings, tall, sizes, rows, feat // pair // strips
    )
    share_second = reduce_ring(links, part_out, n_dp - 1 - ahead)
    share_first = reduce_ring(links, part_lift, ahead)

    def over_seq(share):
        mine = share.astype(BF)
        total = share
        for j in range(1, links.chips):
            total = total + links.out(mine, j * pair).astype(F32)
        mine = total.astype(BF)
        return [mine] if pair == 1 else [mine, links.swap(mine)]

    grad_gate, grad_lift = place_lift(index, over_seq(share_first), sizes)
    grad_out = place_out(index, over_seq(share_second), pair)

    back = attention_backward(packs, grads, part_lift[0])
    done = [back[0]] + [None] * (n_seq - 1)
    for k in order:
        done[k] = links.back(back[k], k)
    d_queries, d_keys, d_values = place_grads(owner_index, done)
    return (d_queries[None], d_keys[None], d_values[None], grad_gate, grad_lift, grad_out)


def solution(mesh):
    in_specs = (
        P("dp", "seq", None),
        P("dp", "seq", None),
        P("dp", "seq", None),
        P("dp", "seq", None),
        P("dp", "seq", None),
        P(),
        P(),
        P("dp", "seq"),
        P("dp"),
        P("dp", None),
        P("dp", None),
        P("dp", None),
    )
    out_specs = (
        P("dp", "seq", None),
        P("dp", "seq", None),
        P("dp", "seq", None),
        P("dp", None),
        P("dp", None),
        P("dp", None),
    )
    return jax.shard_map(step, mesh=mesh, in_specs=in_specs, out_specs=out_specs, check_vma=False)
```
